256 devices in a mesh: member: 8 (over y, core), space: 32 (over z, x).
Axes of the slice: x: 4, y: 4, z: 8, core: 2. Of those that a mesh axis runs over, the one named last changes fastest.
Arguments:
- states: bfloat16 [8, 73, 480, 720], P('member', None, 'space'), may hold values from -6 to 6
- observed: bfloat16 [73, 480, 720], P(None, 'space'), may hold values from -6 to 6
- band_rows: int32 [32], replicated, may hold values from 1 to 15, 361 in all
- encoder_weight: bfloat16 [73, 128], replicated, may hold values from -0.75 to 0.75
- mixing_weight: bfloat16 [128, 128], replicated, may hold values from -0.5 to 0.5
- degree_gain: float32 [368, 128], replicated, may hold values from 0.25 to 2
- decoder_weight: bfloat16 [128, 73], replicated, may hold values from -0.5 to 0.5
Outputs:
- prediction: bfloat16 [8, 73, 480, 720], P('member', None, 'space')
- state_grad: bfloat16 [8, 73, 480, 720], P('member', None, 'space')
The draws below stay inside these ranges and needn't reach their ends.
Inputs may be any that keep to these rules, and one draw needn't show every extreme that they name: Band d holds the next band_rows[d] latitudes, from the north pole southward, in the first rows of the d-th block of 15 rows; the remaining rows of a block are padding, ignored in states and observed. The bands' rows sum to 361, and some band has exactly 15 rows.
All inputs are finite; a program needn't handle non-finite values.
Results may differ from the reference program's by a relative error of at most 0.014.
Values may be sent and summed in bfloat16 or wider, within the bound.
A program may use at most 128 MiB of HBM per device.

```python
import math
import jax
import jax.numpy as jnp
import numpy as np
from jax import lax

NLAT = 361
NLON = 720
LMAX = 360
CH = 128
FIELDS = 73
MEMBERS = 8
BAND = 15
ROWS = 480
MPAD = 384
DEG = 368
N_SPACE = 32


def block_scale(stream_key, extent, shards, least, largest):
    gain = 1.0
    for dim, shards_of in shards:
        draws = jax.random.uniform(jax.random.fold_in(jax.random.fold_in(stream_key, 6), dim), (shards_of,), jnp.float32, least / len(shards), largest / len(shards))
        gain = gain * jnp.repeat(jnp.exp(draws), extent[dim] // shards_of).reshape((-1,) + (1,) * (len(extent) - 1 - dim))
    return gain


def profile(count, total, most, lean):
    portions = [(1 << 20) // math.isqrt(standing ** lean) + 1 for standing in range(2, count + 1)]
    spare, holding = total - most - (count - 1), [1] * (count - 1)
    while spare > 0:
        movable = [i for i in range(count - 1) if holding[i] < most]
        pool, budget = sum([portions[i] for i in movable]), spare
        for i in movable:
            extra = min(most - holding[i], max(1, budget * portions[i] // pool), spare)
            holding[i] = holding[i] + extra
            spare = spare - extra
    return np.array([most] + holding)


def uneven_parts(own_key, count, total, most, skew):
    if count == 2:
        one = jax.random.randint(own_key, (), max(1, total - most), min(most, total - 1) + 1)
        return jnp.stack([one, total - one])
    lengths = jnp.asarray(profile(count, total, most, skew), jnp.int32)
    twos = (count - 1) // 2
    source_of, taker = lengths[1:1 + 2 * twos:2], lengths[2:2 + 2 * twos:2]
    slack = jnp.minimum(source_of - 1, most - taker)
    shifted = jax.random.randint(jax.random.fold_in(own_key, 1), (twos,), 0, 1 << 20) % (slack + 1)
    lengths = lengths.at[1:1 + 2 * twos:2].set(source_of - shifted).at[2:2 + 2 * twos:2].set(taker + shifted)
    return lengths[jax.random.permutation(jax.random.fold_in(own_key, 2), count)]


def centred(stream_key, extent, scale, most, cuts=(), held_as=jnp.bfloat16):
    values = jax.random.normal(stream_key, extent, jnp.float32) * scale
    if len(cuts) > 0:
        values = block_scale(stream_key, extent, cuts, -0.22, 0.18) * values
    return jnp.clip(values, min=-most, max=most).astype(held_as)


def setup_inputs(seed: int = 0) -> dict:
    keys = jax.random.split(jax.random.key(seed), 8)
    states = centred(keys[0], (MEMBERS, FIELDS, ROWS, NLON), 1.0, 6.0, ((0, 8), (2, 32)))
    observed = centred(keys[1], (FIELDS, ROWS, NLON), 1.0, 6.0, ((1, 32),))
    band_rows = uneven_parts(keys[2], N_SPACE, NLAT, BAND, 1).astype(jnp.int32)
    encoder_weight = centred(keys[3], (FIELDS, CH), FIELDS ** -0.5, 0.75)
    mixing_weight = centred(keys[4], (CH, CH), CH ** -0.5, 0.5)
    degree_gain = jnp.clip(jnp.exp(jax.random.uniform(keys[5], (DEG, CH), jnp.float32, math.log(0.25), math.log(2.0))), 0.25, 2.0)
    decoder_weight = centred(keys[6], (CH, FIELDS), CH ** -0.5, 0.5)
    return dict(states=states, observed=observed, band_rows=band_rows, encoder_weight=encoder_weight, mixing_weight=mixing_weight, degree_gain=degree_gain, decoder_weight=decoder_weight)


EPSILON = 1e-05

def row_geometry(band_rows, band_len, lat_count):
    band_count = band_rows.shape[0]
    row_index = jnp.arange(band_count * band_len, dtype=jnp.int32)
    row_owner = row_index // band_len
    offset = row_index - row_owner * band_len
    starts = jnp.cumsum(band_rows) - band_rows
    owner_hot = (row_owner[:, None] == jnp.arange(band_count, dtype=jnp.int32)[None, :]).astype(jnp.int32)
    first_lat = lax.optimization_barrier(jnp.sum(owner_hot * starts[None, :], axis=1))
    length = lax.optimization_barrier(jnp.sum(owner_hot * band_rows[None, :], axis=1))
    live_rows = offset < length
    latitude = jnp.minimum(first_lat + offset, lat_count - 1)
    colatitude = latitude.astype(jnp.float32) * (math.pi / (lat_count - 1))
    return (live_rows, jnp.cos(colatitude), jnp.sin(colatitude))

def diagonal_logs(order_count):
    kvalues = jnp.arange(order_count, dtype=jnp.float32)
    increments = jnp.where(kvalues >= 1.0, 0.5 * jnp.log((2.0 * kvalues + 1.0) / jnp.maximum(2.0 * kvalues, 1.0)), 0.0)
    return 0.5 * math.log(0.5) + jnp.cumsum(increments)

def legendre(orders, log_diag, cosines, sines, top_degree, degrees):
    order_f = orders.astype(jnp.float32)[:, None]
    log_start = log_diag[:, None] + order_f * jnp.log(jnp.maximum(sines, 1e-30))[None, :]
    empty_rows = jnp.zeros((orders.shape[0], cosines.shape[0]), jnp.float32)
    cosine_row = cosines[None, :]

    def recur_block(state_in, block_start):
        first, second, log_scale = state_in
        stacked = []
        for position in range(16):
            degree = block_start + position
            degree_f = degree.astype(jnp.float32)
            past_onset = degree > orders[:, None]
            at_onset = degree == orders[:, None]
            factor_up = jnp.sqrt((4.0 * degree_f * degree_f - 1.0) / jnp.maximum(degree_f * degree_f - order_f * order_f, 1.0))
            factor_back = jnp.sqrt(jnp.maximum((degree_f - 1.0) * (degree_f - 1.0) - order_f * order_f, 0.0) / jnp.maximum(4.0 * (degree_f - 1.0) * (degree_f - 1.0) - 1.0, 1.0))
            current = jnp.where(past_onset, factor_up * (cosine_row * first - factor_back * second), jnp.where(at_onset, 1.0, 0.0))
            magnitude = jnp.maximum(jnp.abs(current), jnp.abs(first))
            factor = jnp.where(magnitude > 1.0, magnitude, 1.0)
            current = current / factor
            previous = first / factor
            log_scale = log_scale + jnp.log(factor)
            keep_mask = (past_onset | at_onset) & (degree <= top_degree)
            stacked.append(jnp.where(keep_mask, current * jnp.exp(log_scale), 0.0))
            second = previous
            first = current
        return ((first, second, log_scale), jnp.stack(stacked))
    block_starts = jnp.arange(degrees // 16, dtype=jnp.int32) * 16
    final_state, legendre_table = lax.scan(recur_block, (empty_rows, empty_rows, log_start), block_starts)
    return legendre_table.reshape(degrees, orders.shape[0], cosines.shape[0])

def transforms(lon_count, order_count, top_degree):
    lon_index = jnp.arange(lon_count, dtype=jnp.int32)
    order_index = jnp.arange(order_count, dtype=jnp.int32)
    angle_table = (order_index[:, None] * lon_index[None, :] % lon_count).astype(jnp.float32) * (2.0 * math.pi / lon_count)
    live_order = (order_index <= top_degree)[:, None]
    cosines = jnp.where(live_order, jnp.cos(angle_table), 0.0)
    sines = jnp.where(live_order, jnp.sin(angle_table), 0.0)
    weight = jnp.where((order_index == 0) | (2 * order_index == lon_count), 1.0, 2.0)[:, None]
    forward = jnp.transpose(jnp.stack([cosines, -sines]), (2, 0, 1)) / lon_count
    inverse = jnp.stack([weight * cosines, -weight * sines])
    return (forward.astype(jnp.bfloat16), inverse.astype(jnp.bfloat16))

def gelu_slope(values):
    return 0.5 * (1.0 + lax.erf(values * (1.0 / math.sqrt(2.0)))) + values * jnp.exp(-0.5 * values * values) * (1.0 / math.sqrt(2.0 * math.pi))

def score_grad(own_fields, everyone, observed, area_weight):
    own_f = own_fields.astype(jnp.float32)
    truth_gap = own_f - observed.astype(jnp.float32)
    truth_dist = jnp.sqrt(lax.optimization_barrier(jnp.sum(truth_gap * truth_gap, axis=0, keepdims=True)) + EPSILON)

    def accumulate(running, other_member):
        member_gap = own_f - other_member.astype(jnp.float32)
        member_dist = jnp.sqrt(lax.optimization_barrier(jnp.sum(member_gap * member_gap, axis=0, keepdims=True)) + EPSILON)
        return (running + member_gap / member_dist, None)
    pair_sum, unused = lax.scan(accumulate, jnp.zeros(own_f.shape, jnp.float32), everyone)
    result = area_weight[None, :, None] * (truth_gap / truth_dist - pair_sum / everyone.shape[0])
    return result.astype(jnp.bfloat16)

def reference(states, observed, band_rows, encoder_weight, mixing_weight, degree_gain, decoder_weight):
    live_rows, cosines, sines = row_geometry(band_rows, BAND, NLAT)
    live_f = live_rows.astype(jnp.float32)
    orders = jnp.arange(MPAD, dtype=jnp.int32)
    legendre_table = legendre(orders, diagonal_logs(MPAD), cosines, sines, LMAX, DEG)
    quad_weight = live_f * sines * (math.pi / (NLAT - 1))
    legendre_forward = (legendre_table * quad_weight[None, None, :]).astype(jnp.bfloat16).astype(jnp.float32)
    legendre_inverse = (legendre_table * live_f[None, None, :]).astype(jnp.bfloat16).astype(jnp.float32)
    fwd_table, inv_table = transforms(NLON, MPAD, LMAX)
    fwd_table = fwd_table.astype(jnp.float32)
    inv_table = inv_table.astype(jnp.float32)
    area_weight = 8.0 * sines * live_f
    enc_f = encoder_weight.astype(jnp.float32)
    mix_f = mixing_weight.astype(jnp.float32)
    dec_f = decoder_weight.astype(jnp.float32)

    def run_forward(member):
        hidden = (jnp.einsum('frl,fc->rlc', member.astype(jnp.float32), enc_f) * live_f[:, None, None]).astype(jnp.bfloat16)
        longitude_modes = jnp.einsum('rlc,lkm->kmrc', hidden.astype(jnp.float32), fwd_table).astype(jnp.bfloat16)
        harmonic_weights = jnp.einsum('ghqn,uhq->guhn', longitude_modes.astype(jnp.float32), legendre_forward).astype(jnp.bfloat16)
        masked_spectrum = (jnp.einsum('klmc,cd->klmd', harmonic_weights.astype(jnp.float32), mix_f) * degree_gain[None, :, None, :]).astype(jnp.bfloat16)
        rebuilt_field = jnp.einsum('pjcx,jco->pcox', masked_spectrum.astype(jnp.float32), legendre_inverse).astype(jnp.bfloat16)
        grid_field = jnp.einsum('kmrc,kml->rlc', rebuilt_field.astype(jnp.float32), inv_table)
        block_out = ((jax.nn.gelu(grid_field, approximate=False) + hidden.astype(jnp.float32)) * live_f[:, None, None]).astype(jnp.bfloat16)
        predicted = (member.astype(jnp.float32) + jnp.einsum('rlc,cf->frl', block_out.astype(jnp.float32), dec_f)) * live_f[None, :, None]
        return (grid_field, predicted.astype(jnp.bfloat16))
    prediction = lax.map(lambda member: run_forward(member)[1], states)
    score_all = lax.map(lambda own_fields: score_grad(own_fields, prediction, observed, area_weight), prediction)

    def run_backward(inputs):
        member, grad_pred = inputs
        grid_field = run_forward(member)[0]
        grad_f = grad_pred.astype(jnp.float32)
        grad_block = jnp.einsum('frl,cf->rlc', grad_f, dec_f)
        grad_field = (grad_block * gelu_slope(grid_field)).astype(jnp.bfloat16)
        rebuilt_gradient = jnp.einsum('rlc,kml->kmrc', grad_field.astype(jnp.float32), inv_table).astype(jnp.bfloat16)
        masked_gradient = jnp.einsum('ghqn,uhq->guhn', rebuilt_gradient.astype(jnp.float32), legendre_inverse)
        grad_scaled = (masked_gradient * degree_gain[None, :, None, :]).astype(jnp.bfloat16)
        harmonic_gradient = jnp.einsum('klmd,cd->klmc', grad_scaled.astype(jnp.float32), mix_f).astype(jnp.bfloat16)
        longitude_gradient = jnp.einsum('sbzv,bze->szev', harmonic_gradient.astype(jnp.float32), legendre_forward).astype(jnp.bfloat16)
        grad_spectral = jnp.einsum('kmrc,lkm->rlc', longitude_gradient.astype(jnp.float32), fwd_table)
        grad_hidden = ((grad_block + grad_spectral) * live_f[:, None, None]).astype(jnp.bfloat16)
        result = (grad_f + jnp.einsum('rlc,fc->frl', grad_hidden.astype(jnp.float32), enc_f)) * live_f[None, :, None]
        return result.astype(jnp.bfloat16)
    state_grad = lax.map(run_backward, (states, score_all))
    return (prediction, state_grad)
```

```python
import functools
import math

import jax
import jax.numpy as jnp
import numpy as np
from jax import lax
from jax.experimental import pallas as pl
from jax.experimental.pallas import tpu as pltpu
from jax.sharding import PartitionSpec as P

NLAT = 361
LMAX = 360
NLON = 720
FIELDS = 73
CH = 128
BAND = 15
BANDS = 32
MEMBERS = 8
MDEV = 12
DEG = 384
PTS = 512
KM = 2 * MDEV
FLAT = 1152
WIDE = BAND * CH

EPSILON = 1e-05
F32 = jnp.float32
BF16 = jnp.bfloat16


def dot(a, b, ca, cb):
    return lax.dot_general(a, b, (((ca,), (cb,)), ((), ())), preferred_element_type=F32)


def params(mb=56):
    return pltpu.CompilerParams(
        vmem_limit_bytes=mb * 1024 * 1024, dimension_semantics=("arbitrary",)
    )


def whole(shape):
    return pl.BlockSpec(shape, lambda *g: (0,) * len(shape))


SMEM = pl.BlockSpec(memory_space=pltpu.SMEM)


def fourier_table():
    orders = np.arange(BANDS * MDEV)
    angle = 2.0 * np.pi * ((orders[:, None] * np.arange(NLON)[None, :]) % NLON) / NLON
    live = (orders <= LMAX)[:, None]
    both = np.stack([np.where(live, np.cos(angle), 0.0), np.where(live, -np.sin(angle), 0.0)])
    both = both.reshape(2, BANDS, MDEV, NLON).transpose(1, 0, 2, 3).reshape(BANDS * KM, NLON)
    return jnp.asarray(both.astype(np.float32), BF16)


def diagonal_logs():
    k = np.arange(1, BANDS * MDEV + 16, dtype=np.float64)
    steps = 0.5 * np.log((2.0 * k + 1.0) / (2.0 * k))
    return np.concatenate([[0.0], np.cumsum(steps)]).astype(np.float32) + np.float32(
        0.5 * math.log(0.5)
    )


def legendre_kernel(first_ref, geo_ref, diag_ref, leg_ref, legt_ref, table):
    step = pl.program_id(0)

    @pl.when(step == 0)
    def _():
        first_order = first_ref[0]
        cosine = jnp.broadcast_to(geo_ref[0:1, :], (16, PTS))
        log_sine = geo_ref[1:2, :]
        live = jnp.broadcast_to(geo_ref[2:3, :], (16, PTS))
        orders = first_order + lax.broadcasted_iota(jnp.int32, (16, 128), 0)
        order_f = orders.astype(F32)
        order_sq = order_f * order_f

        def wide(x):
            return jnp.concatenate([x] * (PTS // 128), axis=1)

        start = wide(diag_ref[...]) + wide(order_f) * log_sine

        def block(number, carry):
            first, second, log_scale = carry
            scale = jnp.exp(log_scale) * live
            for position in range(16):
                degree = number * 16 + position
                lf = jnp.full((16, 128), degree, jnp.int32).astype(F32)
                up = jnp.sqrt((4.0 * lf * lf - 1.0) / jnp.maximum(lf * lf - order_sq, 1.0))
                lb = lf - 1.0
                back = jnp.sqrt(
                    jnp.maximum(lb * lb - order_sq, 0.0) / jnp.maximum(4.0 * lb * lb - 1.0, 1.0)
                )
                up = jnp.where(degree > orders, up, 0.0)
                onset = jnp.where(degree == orders, 1.0, 0.0)
                current = wide(up) * (cosine * first - wide(back) * second) + wide(onset)
                kept = jnp.where(jnp.full((16, PTS), degree, jnp.int32) <= LMAX, current * scale, 0.0)
                for part in range(PTS // 128):
                    table[part, pl.ds(pl.multiple_of(degree * 16, 16), 16), :] = kept[
                        :, part * 128 : part * 128 + 128
                    ]
                second = first
                first = current
            magnitude = jnp.maximum(jnp.abs(first), jnp.abs(second))
            factor = jnp.where(magnitude > 1.0, magnitude, 1.0)
            return first / factor, second / factor, log_scale + jnp.log(factor)

        zero = jnp.zeros((16, PTS), F32)
        lax.fori_loop(0, 23, block, (zero, zero, start))
        table[:, pl.ds(368 * 16, 16 * 16), :] = jnp.zeros((PTS // 128, 256, 128), F32)

    for part in range(PTS // 128):
        lanes = slice(part * 128, part * 128 + 128)
        values = table[part, pl.ds(step, DEG, stride=16), :]
        leg_ref[0, :, lanes] = values.astype(BF16)
        legt_ref[0, lanes, :] = values.T.astype(BF16)


def legendre(first_order, geo, diag):
    return pl.pallas_call(
        legendre_kernel,
        grid=(MDEV,),
        in_specs=[SMEM, whole((8, PTS)), whole((16, 128))],
        out_specs=[
            pl.BlockSpec((1, DEG, PTS), lambda m: (m, 0, 0)),
            pl.BlockSpec((1, PTS, DEG), lambda m: (m, 0, 0)),
        ],
        out_shape=[
            jax.ShapeDtypeStruct((MDEV, DEG, PTS), BF16),
            jax.ShapeDtypeStruct((MDEV, PTS, DEG), BF16),
        ],
        scratch_shapes=[pltpu.VMEM((PTS // 128, DEG * 16, 128), F32)],
        compiler_params=params(),
        name="legendre",
    )(first_order, geo, diag)


def window(row):
    start = row * FIELDS
    return start // 128 * 128, start % 128


def order_factor(first_ref):
    order = first_ref[0] + pl.program_id(0)
    edge = jnp.logical_or(order == 0, order == LMAX)
    return jnp.where(edge, 1.0, 2.0)


def forward_kernel(
    first_ref, z_ref, leg_ref, legt_ref, enc_ref, mix_ref, gain_ref, out_ref, rows, points, made
):
    step = pl.program_id(0)

    @pl.when(step == 0)
    def _():
        for r in range(BAND):
            base, off = window(r)
            pair = z_ref[:, base : base + 256].astype(F32)
            rows[r] = pltpu.roll(pair, (256 - off) % 256, 1)[:, :128]
        points[...] = jnp.zeros((PTS, 256), BF16)

    for r in range(BAND):
        for k in range(2):
            got = rows[r, pl.ds(k * MDEV + step, BANDS, stride=KM), :]
            points[r * BANDS : (r + 1) * BANDS, k * 128 : (k + 1) * 128] = got.astype(BF16)
    coeffs = dot(leg_ref[0], points[...], 1, 0).astype(BF16)
    factor = order_factor(first_ref)
    gain = gain_ref[...] * factor
    filtered = []
    for k in range(2):
        channels = dot(coeffs[:, k * 128 : (k + 1) * 128], enc_ref[...], 1, 0).astype(BF16)
        filtered.append((dot(channels, mix_ref[...], 1, 0) * gain).astype(BF16))
    synth = dot(legt_ref[0], jnp.concatenate(filtered, axis=1), 1, 0)
    for r in range(BAND):
        for k in range(2):
            made[r, pl.ds(k * MDEV + step, BANDS, stride=KM), :] = synth[
                r * BANDS : (r + 1) * BANDS, k * 128 : (k + 1) * 128
            ]

    @pl.when(step == MDEV - 1)
    def _():
        for r in range(BAND):
            out_ref[:, r * CH : (r + 1) * CH] = made[r].astype(BF16)


def backward_kernel(
    first_ref, z_ref, leg_ref, legt_ref, enct_ref, mixt_ref, gain_ref, out_ref, rows, points, made
):
    step = pl.program_id(0)

    @pl.when(step == 0)
    def _():
        for r in range(BAND):
            rows[r] = z_ref[:, r * CH : (r + 1) * CH].astype(F32)
        points[...] = jnp.zeros((PTS, 256), BF16)

    for r in range(BAND):
        for k in range(2):
            got = rows[r, pl.ds(k * MDEV + step, BANDS, stride=KM), :]
            points[r * BANDS : (r + 1) * BANDS, k * 128 : (k + 1) * 128] = got.astype(BF16)
    grads = dot(leg_ref[0], points[...], 1, 0)
    gain = gain_ref[...] * order_factor(first_ref)
    back = []
    for k in range(2):
        scaled = (grads[:, k * 128 : (k + 1) * 128] * gain).astype(BF16)
        channels = dot(scaled, mixt_ref[...], 1, 0).astype(BF16)
        back.append(dot(channels, enct_ref[...], 1, 0).astype(BF16))
    synth = dot(legt_ref[0], jnp.concatenate(back, axis=1), 1, 0)
    for r in range(BAND):
        for k in range(2):
            made[r, pl.ds(k * MDEV + step, BANDS, stride=KM), :] = synth[
                r * BANDS : (r + 1) * BANDS, k * 128 : (k + 1) * 128
            ]

    @pl.when(step == MDEV - 1)
    def _():
        low = jnp.zeros((BANDS * KM, 128), F32)
        at = 0
        for r in range(BAND):
            base, off = window(r)
            while at < base:
                out_ref[:, at : at + 128] = low.astype(BF16)
                low = spill
                at += 128
            value = made[r]
            pair = jnp.concatenate([value, jnp.zeros_like(value)], axis=1)
            moved = pltpu.roll(pair, off, 1)
            low = low + moved[:, :128]
            spill = moved[:, 128:]
        out_ref[:, at : at + 128] = low.astype(BF16)
        at += 128
        out_ref[:, at : at + 128] = spill.astype(BF16)


def spectral(kernel, lanes_out, first_order, z, leg, legt, first_w, second_w, gain):
    return pl.pallas_call(
        kernel,
        grid=(MDEV,),
        in_specs=[
            SMEM,
            whole(z.shape),
            pl.BlockSpec((1, DEG, PTS), lambda m: (m, 0, 0)),
            pl.BlockSpec((1, PTS, DEG), lambda m: (m, 0, 0)),
            whole((128, 128)),
            whole((128, 128)),
            whole((DEG, CH)),
        ],
        out_specs=whole((BANDS * KM, lanes_out)),
        out_shape=jax.ShapeDtypeStruct((BANDS * KM, lanes_out), BF16),
        scratch_shapes=[
            pltpu.VMEM((BAND, BANDS * KM, 128), F32),
            pltpu.VMEM((PTS, 256), BF16),
            pltpu.VMEM((BAND, BANDS * KM, 128), F32),
        ],
        compiler_params=params(),
        name=kernel.__name__,
    )(first_order, z, leg, legt, first_w, second_w, gain)


def grid_kernel(live_ref, s_ref, c_ref, x_ref, enct_ref, dect_ref, pred_ref, slope_ref):
    step = pl.program_id(0)
    for part in range(3):
        lanes = slice(part * CH, (part + 1) * CH)
        field = dot(s_ref[:, lanes], c_ref[...], 0, 0)
        live = live_ref[step * 3 + part]
        state = x_ref[part]
        hidden = (dot(enct_ref[...], state, 1, 0) * live).astype(BF16).astype(F32)
        cdf = 0.5 * (1.0 + lax.erf(field * (1.0 / math.sqrt(2.0))))
        slope = cdf + field * jnp.exp(-0.5 * field * field) * (1.0 / math.sqrt(2.0 * math.pi))
        block = ((field * cdf + hidden) * live).astype(BF16)
        decoded = dot(dect_ref[...], block, 1, 0)
        pred_ref[part] = ((state.astype(F32) + decoded) * live).astype(BF16)
        slope_ref[part] = slope.astype(BF16)


def grid_stage(live, s, c, x, enct, dect):
    return pl.pallas_call(
        grid_kernel,
        grid=(5,),
        in_specs=[
            SMEM,
            pl.BlockSpec((BANDS * KM, 3 * CH), lambda g: (0, g)),
            whole((BANDS * KM, NLON)),
            pl.BlockSpec((3, FIELDS, NLON), lambda g: (g, 0, 0)),
            whole((CH, FIELDS)),
            whole((FIELDS, CH)),
        ],
        out_specs=[
            pl.BlockSpec((3, FIELDS, NLON), lambda g: (g, 0, 0)),
            pl.BlockSpec((3, CH, NLON), lambda g: (g, 0, 0)),
        ],
        out_shape=[
            jax.ShapeDtypeStruct((16, FIELDS, NLON), BF16),
            jax.ShapeDtypeStruct((BAND, CH, NLON), BF16),
        ],
        compiler_params=params(),
        name="grid_stage",
    )(live, s, c, x, enct, dect)


def score_kernel(area_ref, p_ref, o_ref, out_ref):
    area = area_ref[pl.program_id(0)]
    values = [p_ref[e, 0].astype(F32) for e in range(MEMBERS)]
    truth = o_ref[0].astype(F32)

    def inverse(gap):
        return lax.rsqrt(jnp.sum(gap * gap, axis=0, keepdims=True) + EPSILON)

    weights = {}
    for e in range(MEMBERS):
        for f in range(e):
            weights[e, f] = weights[f, e] = inverse(values[e] - values[f]) * (area / MEMBERS)
    for e in range(MEMBERS):
        gap = values[e] - truth
        total = gap * (inverse(gap) * area)
        for f in range(MEMBERS):
            if f != e:
                total = total - (values[e] - values[f]) * weights[e, f]
        out_ref[e, 0] = total.astype(BF16)


def score_stage(area, everyone, truth):
    return pl.pallas_call(
        score_kernel,
        grid=(2, 6),
        in_specs=[
            SMEM,
            pl.BlockSpec((MEMBERS, 1, FIELDS, 128), lambda r, j: (0, r, 0, j)),
            pl.BlockSpec((1, FIELDS, 128), lambda r, j: (r, 0, j)),
        ],
        out_specs=pl.BlockSpec((MEMBERS, 1, FIELDS, 128), lambda r, j: (0, r, 0, j)),
        out_shape=jax.ShapeDtypeStruct((MEMBERS, 2, FIELDS, NLON), BF16),
        compiler_params=pltpu.CompilerParams(dimension_semantics=("arbitrary", "arbitrary")),
        name="score_stage",
    )(area, everyone, truth)


def grad_kernel(g_ref, slope_ref, c_ref, dec_ref, out_ref):
    fields = []
    for part in range(3):
        block = dot(dec_ref[...], g_ref[part], 1, 0)
        fields.append((block * slope_ref[part].astype(F32)).astype(BF16))
    out_ref[...] = dot(c_ref[...], jnp.concatenate(fields, axis=0), 1, 1).astype(BF16)


def grad_stage(score, slope, c, dec):
    return pl.pallas_call(
        grad_kernel,
        grid=(5,),
        in_specs=[
            pl.BlockSpec((3, FIELDS, NLON), lambda g: (g, 0, 0)),
            pl.BlockSpec((3, CH, NLON), lambda g: (g, 0, 0)),
            whole((BANDS * KM, NLON)),
            whole((CH, FIELDS)),
        ],
        out_specs=pl.BlockSpec((BANDS * KM, 3 * CH), lambda g: (0, g)),
        out_shape=jax.ShapeDtypeStruct((BANDS * KM, WIDE), BF16),
        compiler_params=params(),
        name="grad_stage",
    )(score, slope, c, dec)


def final_kernel(weight_ref, live_ref, z_ref, c_ref, g_ref, dec_ref, enc_ref, out_ref, spread):
    spread[...] = dot(z_ref[...], c_ref[...], 0, 0)
    for r in range(BAND):
        score = g_ref[r]
        block = dot(dec_ref[...], score, 1, 0).astype(BF16)
        local = dot(enc_ref[...], block, 1, 0)
        far = spread[r * FIELDS : (r + 1) * FIELDS, :] * weight_ref[r]
        out_ref[r] = ((score.astype(F32) + local + far) * live_ref[r]).astype(BF16)


def final_stage(weight, live, z, c, score, dec, enc):
    return pl.pallas_call(
        final_kernel,
        in_specs=[SMEM, SMEM] + [pl.BlockSpec(memory_space=pltpu.VMEM)] * 5,
        out_specs=pl.BlockSpec(memory_space=pltpu.VMEM),
        out_shape=jax.ShapeDtypeStruct((BAND, FIELDS, NLON), BF16),
        scratch_shapes=[pltpu.VMEM((FLAT, NLON), F32)],
        compiler_params=pltpu.CompilerParams(vmem_limit_bytes=56 * 1024 * 1024),
        name="final_stage",
    )(weight, live, z, c, score, dec, enc)


def exchange(array, axis):
    return lax.all_to_all(array, axis, split_axis=0, concat_axis=0, tiled=True)


def on_device(
    states, observed, band_rows, encoder_weight, mixing_weight, degree_gain, decoder_weight
):
    band = lax.axis_index("space")
    member = lax.axis_index("member")
    first = band * MDEV

    number = jnp.arange(BANDS, dtype=jnp.int32)
    point = jnp.arange(PTS, dtype=jnp.int32)
    point_band, point_row = point % BANDS, point // BANDS
    starts = jnp.sum(jnp.where(number[:, None] < point_band[None], band_rows[:, None], 0), axis=0)
    counts = jnp.sum(jnp.where(number[:, None] == point_band[None], band_rows[:, None], 0), axis=0)
    colatitude = jnp.minimum(starts + point_row, NLAT - 1).astype(F32) * (math.pi / (NLAT - 1))
    log_sine = jnp.log(jnp.maximum(jnp.sin(colatitude), 1e-30))
    live = (point_row < counts).astype(F32)
    zero = jnp.zeros_like(live)
    geo = jnp.stack([jnp.cos(colatitude), log_sine, live] + [zero] * 5)
    own_start = jnp.sum(jnp.where(number < band, band_rows, 0))
    own_count = jnp.sum(jnp.where(number == band, band_rows, 0))
    row = jnp.arange(16, dtype=jnp.int32)
    own_live = (row < own_count).astype(F32)
    own_lat = jnp.minimum(own_start + row, NLAT - 1).astype(F32) * (math.pi / (NLAT - 1))
    own_sine = jnp.sin(own_lat)
    own_weight = own_live * own_sine * (math.pi / (NLAT - 1) / NLON)
    own_area = 8.0 * own_sine * own_live
    first_order = first.reshape(1)

    c = fourier_table()
    diag = lax.dynamic_slice_in_dim(jnp.asarray(diagonal_logs()), first, 16)
    diag = jnp.broadcast_to(diag[:, None], (16, 128))
    gain = jnp.pad(degree_gain, ((0, DEG - degree_gain.shape[0]), (0, 0)))
    enc = encoder_weight
    enct = enc.T
    dec = decoder_weight
    dect = dec.T
    enc_wide = jnp.pad(enc, ((0, 128 - FIELDS), (0, 0)))
    enct_wide = enc_wide.T

    x = jnp.transpose(states[0], (1, 0, 2))
    flat = jnp.pad(x.reshape(BAND * FIELDS, NLON), ((0, FLAT - BAND * FIELDS), (0, 0)))
    lane_row = jnp.arange(FLAT, dtype=jnp.int32) // FIELDS
    lane_weight = jnp.sum(jnp.where(row[:, None] == lane_row[None], own_weight[:, None], 0.0), axis=0)
    zonal = (
        jnp.einsum("aj,bj->ab", c, flat, preferred_element_type=F32) * lane_weight[None]
    ).astype(BF16)

    arrived = exchange(zonal, "space")
    leg, legt = legendre(first_order, geo, diag)
    synth = spectral(
        forward_kernel, WIDE, first_order, arrived, leg, legt, enc_wide, mixing_weight, gain
    )
    synth = exchange(synth, "space")
    predicted, slope = grid_stage(own_live, synth, c, x, enct, dect)

    everyone = exchange(predicted, "member").reshape(MEMBERS, 2, FIELDS, NLON)
    padded = jnp.pad(observed, ((0, 0), (0, 1), (0, 0)))
    truth = jnp.transpose(lax.dynamic_slice_in_dim(padded, member * 2, 2, 1), (1, 0, 2))
    area = lax.dynamic_slice_in_dim(own_area, member * 2, 2)
    share = score_stage(area, everyone, truth)
    score = exchange(share.reshape(16, FIELDS, NLON), "member")

    grads = exchange(grad_stage(score, slope, c, dec), "space")
    grads = spectral(
        backward_kernel, FLAT, first_order, grads, leg, legt, enct_wide, mixing_weight.T, gain
    )
    grads = exchange(grads, "space")
    result = final_stage(own_weight, own_live, grads, c, score, dec, enc)
    prediction = jnp.transpose(predicted[:BAND], (1, 0, 2))[None]
    return (prediction, jnp.transpose(result, (1, 0, 2))[None])


def solution(mesh):
    in_specs = (P("member", None, "space", None), P(None, "space", None), P(), P(), P(), P(), P())
    out_specs = (P("member", None, "space", None), P("member", None, "space", None))
    return jax.shard_map(
        on_device, mesh=mesh, in_specs=in_specs, out_specs=out_specs, check_vma=False
    )
```

```python
import functools
import math

import jax
import jax.numpy as jnp
import numpy as np
from jax import lax
from jax.experimental import pallas as pl
from jax.experimental.pallas import tpu as pltpu
from jax.sharding import PartitionSpec as P

NLAT = 361
LMAX = 360
NLON = 720
FIELDS = 73
CH = 128
BAND = 15
BANDS = 32
MEMBERS = 8
MDEV = 12
DEG = 384
PTS = 512
KM = 2 * MDEV
GROUPS = 3
GM = MDEV // GROUPS
GK = 2 * GM
MESH = pl.DeviceIdType.MESH
FLAT = 1152
WIDE = BAND * CH

EPSILON = 1e-05
F32 = jnp.float32
BF16 = jnp.bfloat16


def dot(a, b, ca, cb):
    return lax.dot_general(a, b, (((ca,), (cb,)), ((), ())), preferred_element_type=F32)


def params(mb=56):
    return pltpu.CompilerParams(
        vmem_limit_bytes=mb * 1024 * 1024, dimension_semantics=("arbitrary",)
    )


def whole(shape):
    return pl.BlockSpec(shape, lambda *g: (0,) * len(shape))


SMEM = pl.BlockSpec(memory_space=pltpu.SMEM)


def fourier_table():
    orders = np.arange(BANDS * MDEV)
    angle = 2.0 * np.pi * ((orders[:, None] * np.arange(NLON)[None, :]) % NLON) / NLON
    live = (orders <= LMAX)[:, None]
    both = np.stack([np.where(live, np.cos(angle), 0.0), np.where(live, -np.sin(angle), 0.0)])
    both = both.reshape(2, BANDS, GROUPS, GM, NLON).transpose(2, 1, 0, 3, 4)
    both = both.reshape(BANDS * KM, NLON)
    return jnp.asarray(both.astype(np.float32), BF16)


def diagonal_logs():
    k = np.arange(1, BANDS * MDEV + 16, dtype=np.float64)
    steps = 0.5 * np.log((2.0 * k + 1.0) / (2.0 * k))
    return np.concatenate([[0.0], np.cumsum(steps)]).astype(np.float32) + np.float32(
        0.5 * math.log(0.5)
    )


def legendre_rows(first_order, geo_ref, diag_ref, table):
    cosine = jnp.broadcast_to(geo_ref[0:1, :], (16, PTS))
    log_sine = geo_ref[1:2, :]
    live = jnp.broadcast_to(geo_ref[2:3, :], (16, PTS))
    orders = first_order + lax.broadcasted_iota(jnp.int32, (16, 128), 0)
    order_f = orders.astype(F32)
    order_sq = order_f * order_f

    def wide(x):
        return jnp.concatenate([x] * (PTS // 128), axis=1)

    start = wide(diag_ref[...]) + wide(order_f) * log_sine

    def block(number, carry):
        first, second, log_scale = carry
        scale = jnp.exp(log_scale) * live
        for position in range(16):
            degree = number * 16 + position
            lf = jnp.full((16, 128), degree, jnp.int32).astype(F32)
            up = jnp.sqrt((4.0 * lf * lf - 1.0) / jnp.maximum(lf * lf - order_sq, 1.0))
            lb = lf - 1.0
            back = jnp.sqrt(
                jnp.maximum(lb * lb - order_sq, 0.0) / jnp.maximum(4.0 * lb * lb - 1.0, 1.0)
            )
            up = jnp.where(degree > orders, up, 0.0)
            onset = jnp.where(degree == orders, 1.0, 0.0)
            current = wide(up) * (cosine * first - wide(back) * second) + wide(onset)
            kept = jnp.where(jnp.full((16, PTS), degree, jnp.int32) <= LMAX, current * scale, 0.0)
            for part in range(PTS // 128):
                table[part, pl.ds(pl.multiple_of(degree * 16, 16), 16), :] = kept[
                    :, part * 128 : part * 128 + 128
                ]
            second = first
            first = current
        magnitude = jnp.maximum(jnp.abs(first), jnp.abs(second))
        factor = jnp.where(magnitude > 1.0, magnitude, 1.0)
        return first / factor, second / factor, log_scale + jnp.log(factor)

    zero = jnp.zeros((16, PTS), F32)
    lax.fori_loop(0, 23, block, (zero, zero, start))
    table[:, pl.ds(368 * 16, 16 * 16), :] = jnp.zeros((PTS // 128, 256, 128), F32)


def legendre_tables(table, leg, legt):
    def one(m, carry):
        for part in range(PTS // 128):
            lanes = slice(part * 128, part * 128 + 128)
            values = table[part, pl.ds(m, DEG, stride=16), :]
            leg[m, :, lanes] = values.astype(BF16)
            legt[m, lanes, :] = values.T.astype(BF16)
        return carry

    lax.fori_loop(0, MDEV, one, 0)


def window(row):
    start = row * FIELDS
    return start // 128 * 128, start % 128


def enter():
    band, member = lax.axis_index("space"), lax.axis_index("member")
    barrier = pltpu.get_barrier_semaphore()

    def signal(i, carry):
        peer = lax.rem(band + i, BANDS)
        pl.semaphore_signal(barrier, inc=1, device_id=(member, peer), device_id_type=MESH)
        return carry

    lax.fori_loop(1, BANDS, signal, 0)
    pl.semaphore_wait(barrier, BANDS - 1)


def send_group(source, target, group, sent, got):
    band, member = lax.axis_index("space"), lax.axis_index("member")

    def send(i, carry):
        peer = lax.rem(band + i, BANDS)
        pltpu.make_async_remote_copy(
            src_ref=source.at[group, peer],
            dst_ref=target.at[group, band],
            send_sem=sent.at[group],
            recv_sem=got.at[group],
            device_id=(member, peer),
            device_id_type=MESH,
        ).start()
        return carry

    lax.fori_loop(1, BANDS, send, 0)
    pltpu.make_async_copy(source.at[group, band], target.at[group, band], got.at[group]).start()


def wait_arrived(source, target, group, got):
    pltpu.make_async_copy(source.at[group], target.at[group], got.at[group]).wait()


def wait_sent(source, target, group, sent):
    most = pl.ds(0, BANDS - 1)
    pltpu.make_async_copy(
        source.at[group, most], target.at[group, most], sent.at[group]
    ).wait()


def gather_points(rows, points, order):
    for r in range(BAND):
        for k in range(2):
            got = rows[r, pl.ds(k * GM + order, BANDS, stride=GK), :]
            points[r * BANDS : (r + 1) * BANDS, k * 128 : (k + 1) * 128] = got.astype(BF16)


def scatter_points(synth, made, order):
    for r in range(BAND):
        for k in range(2):
            made[r, pl.ds(k * GM + order, BANDS, stride=GK), :] = synth[
                r * BANDS : (r + 1) * BANDS, k * 128 : (k + 1) * 128
            ]


def order_factor(order):
    return jnp.where(jnp.logical_or(order == 0, order == LMAX), 1.0, 2.0)


def forward_kernel(
    geo_ref, diag_ref, enc_ref, mix_ref, gain_ref, z_ref, out_ref, leg_out, legt_out,
    table, leg, legt, arrived, rows, points, made, ready, sent_in, got_in, sent_out, got_out, kept
):
    first_order = lax.axis_index("space") * MDEV
    enter()
    for group in range(GROUPS):
        send_group(z_ref, arrived, group, sent_in, got_in)
    legendre_rows(first_order, geo_ref, diag_ref, table)
    legendre_tables(table, leg, legt)
    save = pltpu.make_async_copy(leg, leg_out, kept.at[0])
    save_t = pltpu.make_async_copy(legt, legt_out, kept.at[1])
    save.start()
    save_t.start()
    points[...] = jnp.zeros((PTS, 256), BF16)

    def one_group(group, carry):
        wait_arrived(z_ref, arrived, group, got_in)
        for r in range(BAND):
            base, off = window(r)
            pair = arrived[group, :, :, base : base + 256].astype(F32).reshape(BANDS * GK, 256)
            rows[r] = pltpu.roll(pair, (256 - off) % 256, 1)[:, :128]

        def one_order(order, carry):
            m = group * GM + order
            gather_points(rows, points, order)
            coeffs = dot(leg[m], points[...], 1, 0).astype(BF16)
            gain = gain_ref[...] * order_factor(first_order + m)
            filtered = []
            for k in range(2):
                channels = dot(coeffs[:, k * 128 : (k + 1) * 128], enc_ref[...], 1, 0).astype(BF16)
                filtered.append((dot(channels, mix_ref[...], 1, 0) * gain).astype(BF16))
            scatter_points(dot(legt[m], jnp.concatenate(filtered, axis=1), 1, 0), made, order)
            return carry

        lax.fori_loop(0, GM, one_order, 0)
        for r in range(BAND):
            ready[group, :, :, r * CH : (r + 1) * CH] = (
                made[r].reshape(BANDS, GK, CH).astype(BF16)
            )
        send_group(ready, out_ref, group, sent_out, got_out)
        return carry

    lax.fori_loop(0, GROUPS, one_group, 0)
    save.wait()
    save_t.wait()
    for group in range(GROUPS):
        wait_sent(z_ref, arrived, group, sent_in)
        wait_sent(ready, out_ref, group, sent_out)
        wait_arrived(ready, out_ref, group, got_out)


def backward_kernel(
    enct_ref, mixt_ref, gain_ref, leg_in, legt_in, z_ref, out_ref,
    leg, legt, arrived, rows, points, made, ready, sent_in, got_in, sent_out, got_out, kept
):
    first_order = lax.axis_index("space") * MDEV
    load = pltpu.make_async_copy(leg_in, leg, kept.at[0])
    load_t = pltpu.make_async_copy(legt_in, legt, kept.at[1])
    load.start()
    load_t.start()
    enter()
    for group in range(GROUPS):
        send_group(z_ref, arrived, group, sent_in, got_in)
    points[...] = jnp.zeros((PTS, 256), BF16)
    load.wait()
    load_t.wait()

    def one_group(group, carry):
        wait_arrived(z_ref, arrived, group, got_in)
        for r in range(BAND):
            rows[r] = (
                arrived[group, :, :, r * CH : (r + 1) * CH].astype(F32).reshape(BANDS * GK, CH)
            )

        def one_order(order, carry):
            m = group * GM + order
            gather_points(rows, points, order)
            grads = dot(leg[m], points[...], 1, 0)
            gain = gain_ref[...] * order_factor(first_order + m)
            back = []
            for k in range(2):
                scaled = (grads[:, k * 128 : (k + 1) * 128] * gain).astype(BF16)
                channels = dot(scaled, mixt_ref[...], 1, 0).astype(BF16)
                back.append(dot(channels, enct_ref[...], 1, 0).astype(BF16))
            scatter_points(dot(legt[m], jnp.concatenate(back, axis=1), 1, 0), made, order)
            return carry

        lax.fori_loop(0, GM, one_order, 0)

        def put(at, value):
            ready[group, :, :, at : at + 128] = value.reshape(BANDS, GK, 128).astype(BF16)

        low = spill = jnp.zeros((BANDS * GK, 128), F32)
        at = 0
        for r in range(BAND):
            base, off = window(r)
            while at < base:
                put(at, low)
                low = spill
                at += 128
            value = made[r]
            moved = pltpu.roll(jnp.concatenate([value, jnp.zeros_like(value)], axis=1), off, 1)
            low = low + moved[:, :128]
            spill = moved[:, 128:]
        put(at, low)
        put(at + 128, spill)
        send_group(ready, out_ref, group, sent_out, got_out)
        return carry

    lax.fori_loop(0, GROUPS, one_group, 0)
    for group in range(GROUPS):
        wait_sent(z_ref, arrived, group, sent_in)
        wait_sent(ready, out_ref, group, sent_out)
        wait_arrived(ready, out_ref, group, got_out)


VMEM = pl.BlockSpec(memory_space=pltpu.VMEM)
ANY = pl.BlockSpec(memory_space=pl.ANY)
LEG = jax.ShapeDtypeStruct((MDEV, DEG, PTS), BF16)
LEGT = jax.ShapeDtypeStruct((MDEV, PTS, DEG), BF16)


def chunks(lanes):
    return (GROUPS, BANDS, GK, lanes)


def spectral_scratch(lanes_in, lanes_out):
    return [
        pltpu.VMEM(LEG.shape, BF16),
        pltpu.VMEM(LEGT.shape, BF16),
        pltpu.VMEM(chunks(lanes_in), BF16),
        pltpu.VMEM((BAND, BANDS * GK, 128), F32),
        pltpu.VMEM((PTS, 256), BF16),
        pltpu.VMEM((BAND, BANDS * GK, 128), F32),
        pltpu.VMEM(chunks(lanes_out), BF16),
    ] + [pltpu.SemaphoreType.DMA((GROUPS,))] * 4 + [pltpu.SemaphoreType.DMA((2,))]


def remote_params(collective):
    return pltpu.CompilerParams(
        collective_id=collective, vmem_limit_bytes=58 * 1024 * 1024, has_side_effects=True
    )


def forward(geo, diag, enc, mix, gain, z):
    return pl.pallas_call(
        forward_kernel,
        in_specs=[VMEM] * 6,
        out_specs=[ANY] * 3,
        out_shape=[jax.ShapeDtypeStruct(chunks(WIDE), BF16), LEG, LEGT],
        scratch_shapes=[pltpu.VMEM((PTS // 128, DEG * 16, 128), F32)]
        + spectral_scratch(FLAT, WIDE),
        compiler_params=remote_params(1),
        name="forward",
    )(geo, diag, enc, mix, gain, z)


def backward(enct, mixt, gain, leg, legt, z):
    return pl.pallas_call(
        backward_kernel,
        in_specs=[VMEM] * 3 + [ANY] * 2 + [VMEM],
        out_specs=ANY,
        out_shape=jax.ShapeDtypeStruct(chunks(FLAT), BF16),
        scratch_shapes=spectral_scratch(WIDE, FLAT),
        compiler_params=remote_params(2),
        name="backward",
    )(enct, mixt, gain, leg, legt, z)


def grid_kernel(live_ref, s_ref, c_ref, x_ref, enct_ref, dect_ref, pred_ref, slope_ref):
    step = pl.program_id(0)
    for part in range(3):
        lanes = slice(part * CH, (part + 1) * CH)
        field = dot(s_ref[:, lanes], c_ref[...], 0, 0)
        live = live_ref[step * 3 + part]
        state = x_ref[part]
        hidden = (dot(enct_ref[...], state, 1, 0) * live).astype(BF16).astype(F32)
        cdf = 0.5 * (1.0 + lax.erf(field * (1.0 / math.sqrt(2.0))))
        slope = cdf + field * jnp.exp(-0.5 * field * field) * (1.0 / math.sqrt(2.0 * math.pi))
        block = ((field * cdf + hidden) * live).astype(BF16)
        decoded = dot(dect_ref[...], block, 1, 0)
        pred_ref[part] = ((state.astype(F32) + decoded) * live).astype(BF16)
        slope_ref[part] = slope.astype(BF16)


def grid_stage(live, s, c, x, enct, dect):
    return pl.pallas_call(
        grid_kernel,
        grid=(5,),
        in_specs=[
            SMEM,
            pl.BlockSpec((BANDS * KM, 3 * CH), lambda g: (0, g)),
            whole((BANDS * KM, NLON)),
            pl.BlockSpec((3, FIELDS, NLON), lambda g: (g, 0, 0)),
            whole((CH, FIELDS)),
            whole((FIELDS, CH)),
        ],
        out_specs=[
            pl.BlockSpec((3, FIELDS, NLON), lambda g: (g, 0, 0)),
            pl.BlockSpec((3, CH, NLON), lambda g: (g, 0, 0)),
        ],
        out_shape=[
            jax.ShapeDtypeStruct((16, FIELDS, NLON), BF16),
            jax.ShapeDtypeStruct((BAND, CH, NLON), BF16),
        ],
        compiler_params=params(),
        name="grid_stage",
    )(live, s, c, x, enct, dect)


def score_kernel(area_ref, p_ref, o_ref, out_ref):
    area = area_ref[pl.program_id(0)]
    values = [p_ref[e, 0].astype(F32) for e in range(MEMBERS)]
    truth = o_ref[0].astype(F32)

    def inverse(gap):
        return lax.rsqrt(jnp.sum(gap * gap, axis=0, keepdims=True) + EPSILON)

    weights = {}
    for e in range(MEMBERS):
        for f in range(e):
            weights[e, f] = weights[f, e] = inverse(values[e] - values[f]) * (area / MEMBERS)
    for e in range(MEMBERS):
        gap = values[e] - truth
        total = gap * (inverse(gap) * area)
        for f in range(MEMBERS):
            if f != e:
                total = total - (values[e] - values[f]) * weights[e, f]
        out_ref[e, 0] = total.astype(BF16)


def score_stage(area, everyone, truth):
    return pl.pallas_call(
        score_kernel,
        grid=(2, 6),
        in_specs=[
            SMEM,
            pl.BlockSpec((MEMBERS, 1, FIELDS, 128), lambda r, j: (0, r, 0, j)),
            pl.BlockSpec((1, FIELDS, 128), lambda r, j: (r, 0, j)),
        ],
        out_specs=pl.BlockSpec((MEMBERS, 1, FIELDS, 128), lambda r, j: (0, r, 0, j)),
        out_shape=jax.ShapeDtypeStruct((MEMBERS, 2, FIELDS, NLON), BF16),
        compiler_params=pltpu.CompilerParams(dimension_semantics=("arbitrary", "arbitrary")),
        name="score_stage",
    )(area, everyone, truth)


def grad_kernel(g_ref, slope_ref, c_ref, dec_ref, out_ref):
    fields = []
    for part in range(3):
        block = dot(dec_ref[...], g_ref[part], 1, 0)
        fields.append((block * slope_ref[part].astype(F32)).astype(BF16))
    out_ref[...] = dot(c_ref[...], jnp.concatenate(fields, axis=0), 1, 1).astype(BF16)


def grad_stage(score, slope, c, dec):
    return pl.pallas_call(
        grad_kernel,
        grid=(5,),
        in_specs=[
            pl.BlockSpec((3, FIELDS, NLON), lambda g: (g, 0, 0)),
            pl.BlockSpec((3, CH, NLON), lambda g: (g, 0, 0)),
            whole((BANDS * KM, NLON)),
            whole((CH, FIELDS)),
        ],
        out_specs=pl.BlockSpec((BANDS * KM, 3 * CH), lambda g: (0, g)),
        out_shape=jax.ShapeDtypeStruct((BANDS * KM, WIDE), BF16),
        compiler_params=params(),
        name="grad_stage",
    )(score, slope, c, dec)


def final_kernel(weight_ref, live_ref, z_ref, c_ref, g_ref, dec_ref, enc_ref, out_ref, spread):
    spread[...] = dot(z_ref[...], c_ref[...], 0, 0)
    for r in range(BAND):
        score = g_ref[r]
        block = dot(dec_ref[...], score, 1, 0).astype(BF16)
        local = dot(enc_ref[...], block, 1, 0)
        far = spread[r * FIELDS : (r + 1) * FIELDS, :] * weight_ref[r]
        out_ref[r] = ((score.astype(F32) + local + far) * live_ref[r]).astype(BF16)


def final_stage(weight, live, z, c, score, dec, enc):
    return pl.pallas_call(
        final_kernel,
        in_specs=[SMEM, SMEM] + [pl.BlockSpec(memory_space=pltpu.VMEM)] * 5,
        out_specs=pl.BlockSpec(memory_space=pltpu.VMEM),
        out_shape=jax.ShapeDtypeStruct((BAND, FIELDS, NLON), BF16),
        scratch_shapes=[pltpu.VMEM((FLAT, NLON), F32)],
        compiler_params=pltpu.CompilerParams(vmem_limit_bytes=56 * 1024 * 1024),
        name="final_stage",
    )(weight, live, z, c, score, dec, enc)


def exchange(array, axis):
    return lax.all_to_all(array, axis, split_axis=0, concat_axis=0, tiled=True)


def on_device(
    states, observed, band_rows, encoder_weight, mixing_weight, degree_gain, decoder_weight
):
    band = lax.axis_index("space")
    member = lax.axis_index("member")
    first = band * MDEV

    number = jnp.arange(BANDS, dtype=jnp.int32)
    point = jnp.arange(PTS, dtype=jnp.int32)
    point_band, point_row = point % BANDS, point // BANDS
    starts = jnp.sum(jnp.where(number[:, None] < point_band[None], band_rows[:, None], 0), axis=0)
    counts = jnp.sum(jnp.where(number[:, None] == point_band[None], band_rows[:, None], 0), axis=0)
    colatitude = jnp.minimum(starts + point_row, NLAT - 1).astype(F32) * (math.pi / (NLAT - 1))
    log_sine = jnp.log(jnp.maximum(jnp.sin(colatitude), 1e-30))
    live = (point_row < counts).astype(F32)
    zero = jnp.zeros_like(live)
    geo = jnp.stack([jnp.cos(colatitude), log_sine, live] + [zero] * 5)
    own_start = jnp.sum(jnp.where(number < band, band_rows, 0))
    own_count = jnp.sum(jnp.where(number == band, band_rows, 0))
    row = jnp.arange(16, dtype=jnp.int32)
    own_live = (row < own_count).astype(F32)
    own_lat = jnp.minimum(own_start + row, NLAT - 1).astype(F32) * (math.pi / (NLAT - 1))
    own_sine = jnp.sin(own_lat)
    own_weight = own_live * own_sine * (math.pi / (NLAT - 1) / NLON)
    own_area = 8.0 * own_sine * own_live

    c = fourier_table()
    diag = lax.dynamic_slice_in_dim(jnp.asarray(diagonal_logs()), first, 16)
    diag = jnp.broadcast_to(diag[:, None], (16, 128))
    gain = jnp.pad(degree_gain, ((0, DEG - degree_gain.shape[0]), (0, 0)))
    enc = encoder_weight
    enct = enc.T
    dec = decoder_weight
    dect = dec.T
    enc_wide = jnp.pad(enc, ((0, 128 - FIELDS), (0, 0)))
    enct_wide = enc_wide.T

    x = jnp.transpose(states[0], (1, 0, 2))
    flat = jnp.pad(x.reshape(BAND * FIELDS, NLON), ((0, FLAT - BAND * FIELDS), (0, 0)))
    lane_row = jnp.arange(FLAT, dtype=jnp.int32) // FIELDS
    lane_weight = jnp.sum(jnp.where(row[:, None] == lane_row[None], own_weight[:, None], 0.0), axis=0)
    zonal = (
        jnp.einsum("aj,bj->ab", c, flat, preferred_element_type=F32) * lane_weight[None]
    ).astype(BF16)

    synth, leg, legt = forward(geo, diag, enc_wide, mixing_weight, gain, zonal.reshape(chunks(FLAT)))
    synth = synth.reshape(BANDS * KM, WIDE)
    predicted, slope = grid_stage(own_live, synth, c, x, enct, dect)

    everyone = exchange(predicted, "member").reshape(MEMBERS, 2, FIELDS, NLON)
    padded = jnp.pad(observed, ((0, 0), (0, 1), (0, 0)))
    truth = jnp.transpose(lax.dynamic_slice_in_dim(padded, member * 2, 2, 1), (1, 0, 2))
    area = lax.dynamic_slice_in_dim(own_area, member * 2, 2)
    share = score_stage(area, everyone, truth)
    score = exchange(share.reshape(16, FIELDS, NLON), "member")

    grads = grad_stage(score, slope, c, dec).reshape(chunks(WIDE))
    grads = backward(enct_wide, mixing_weight.T, gain, leg, legt, grads)
    grads = grads.reshape(BANDS * KM, FLAT)
    result = final_stage(own_weight, own_live, grads, c, score, dec, enc)
    prediction = jnp.transpose(predicted[:BAND], (1, 0, 2))[None]
    return (prediction, jnp.transpose(result, (1, 0, 2))[None])


def solution(mesh):
    in_specs = (P("member", None, "space", None), P(None, "space", None), P(), P(), P(), P(), P())
    out_specs = (P("member", None, "space", None), P("member", None, "space", None))
    return jax.shard_map(
        on_device, mesh=mesh, in_specs=in_specs, out_specs=out_specs, check_vma=False
    )
```

```python
import math

import jax
import jax.numpy as jnp
import numpy as np
from jax import lax
from jax.experimental import pallas as pl
from jax.experimental.pallas import tpu as pltpu
from jax.sharding import PartitionSpec as P

NLAT = 361
LMAX = 360
NLON = 720
FIELDS = 73
CH = 128
BAND = 15
BANDS = 32
MEMBERS = 8
MDEV = 12
DEG = 384
PTS = 512
KM = 2 * MDEV
GROUPS = 3
GM = MDEV // GROUPS
GK = 2 * GM
MESH = pl.DeviceIdType.MESH
FLAT = 1152
WIDE = BAND * CH

EPSILON = 1e-05
F32 = jnp.float32
BF16 = jnp.bfloat16


def dot(a, b, ca, cb):
    return lax.dot_general(a, b, (((ca,), (cb,)), ((), ())), preferred_element_type=F32)


SMEM = pl.BlockSpec(memory_space=pltpu.SMEM)


def fourier_table():
    orders = np.arange(BANDS * MDEV)
    angle = 2.0 * np.pi * ((orders[:, None] * np.arange(NLON)[None, :]) % NLON) / NLON
    live = (orders <= LMAX)[:, None]
    both = np.stack([np.where(live, np.cos(angle), 0.0), np.where(live, -np.sin(angle), 0.0)])
    both = both.reshape(2, BANDS, GROUPS, GM, NLON).transpose(2, 1, 0, 3, 4)
    both = both.reshape(BANDS * KM, NLON)
    return jnp.asarray(both.astype(np.float32), BF16)


def diagonal_logs():
    k = np.arange(1, BANDS * MDEV + 16, dtype=np.float64)
    steps = 0.5 * np.log((2.0 * k + 1.0) / (2.0 * k))
    return np.concatenate([[0.0], np.cumsum(steps)]).astype(np.float32) + np.float32(
        0.5 * math.log(0.5)
    )


def legendre_rows(first_order, geo_ref, diag_ref, table):
    cosine = jnp.broadcast_to(geo_ref[0:1, :], (16, PTS))
    log_sine = geo_ref[1:2, :]
    live = jnp.broadcast_to(geo_ref[2:3, :], (16, PTS))
    orders = first_order + lax.broadcasted_iota(jnp.int32, (16, 128), 0)
    order_f = orders.astype(F32)
    order_sq = order_f * order_f

    def wide(x):
        return jnp.concatenate([x] * (PTS // 128), axis=1)

    start = wide(diag_ref[...]) + wide(order_f) * log_sine

    def block(number, carry):
        first, second, log_scale = carry
        scale = jnp.exp(log_scale) * live
        for position in range(16):
            degree = number * 16 + position
            lf = jnp.full((16, 128), degree, jnp.int32).astype(F32)
            up = jnp.sqrt((4.0 * lf * lf - 1.0) / jnp.maximum(lf * lf - order_sq, 1.0))
            lb = lf - 1.0
            back = jnp.sqrt(
                jnp.maximum(lb * lb - order_sq, 0.0) / jnp.maximum(4.0 * lb * lb - 1.0, 1.0)
            )
            up = jnp.where(degree > orders, up, 0.0)
            onset = jnp.where(degree == orders, 1.0, 0.0)
            current = wide(up) * (cosine * first - wide(back) * second) + wide(onset)
            kept = jnp.where(jnp.full((16, PTS), degree, jnp.int32) <= LMAX, current * scale, 0.0)
            for part in range(PTS // 128):
                table[part, pl.ds(pl.multiple_of(degree * 16, 16), 16), :] = kept[
                    :, part * 128 : part * 128 + 128
                ]
            second = first
            first = current
        magnitude = jnp.maximum(jnp.abs(first), jnp.abs(second))
        factor = jnp.where(magnitude > 1.0, magnitude, 1.0)
        return first / factor, second / factor, log_scale + jnp.log(factor)

    zero = jnp.zeros((16, PTS), F32)
    lax.fori_loop(0, 23, block, (zero, zero, start))
    table[:, pl.ds(368 * 16, 16 * 16), :] = jnp.zeros((PTS // 128, 256, 128), F32)


def legendre_tables(table, leg, legt):
    def one(m, carry):
        for part in range(PTS // 128):
            lanes = slice(part * 128, part * 128 + 128)
            values = table[part, pl.ds(m, DEG, stride=16), :]
            leg[m, :, lanes] = values.astype(BF16)
            legt[m, lanes, :] = values.T.astype(BF16)
        return carry

    lax.fori_loop(0, MDEV, one, 0)


def window(row):
    start = row * FIELDS
    return start // 128 * 128, start % 128


def enter():
    band, member = lax.axis_index("space"), lax.axis_index("member")
    barrier = pltpu.get_barrier_semaphore()

    def signal(i, carry):
        peer = lax.rem(band + i, BANDS)
        pl.semaphore_signal(barrier, inc=1, device_id=(member, peer), device_id_type=MESH)
        return carry

    lax.fori_loop(1, BANDS, signal, 0)
    pl.semaphore_wait(barrier, BANDS - 1)


def send_group(source, target, group, sent, got):
    band, member = lax.axis_index("space"), lax.axis_index("member")

    def send(i, carry):
        peer = lax.rem(band + i, BANDS)
        pltpu.make_async_remote_copy(
            src_ref=source.at[group, peer],
            dst_ref=target.at[group, band],
            send_sem=sent.at[group],
            recv_sem=got.at[group],
            device_id=(member, peer),
            device_id_type=MESH,
        ).start()
        return carry

    lax.fori_loop(1, BANDS, send, 0)
    pltpu.make_async_copy(source.at[group, band], target.at[group, band], got.at[group]).start()


def wait_arrived(source, target, group, got):
    pltpu.make_async_copy(source.at[group], target.at[group], got.at[group]).wait()


def wait_sent(source, target, group, sent):
    most = pl.ds(0, BANDS - 1)
    pltpu.make_async_copy(
        source.at[group, most], target.at[group, most], sent.at[group]
    ).wait()


def gather_points(rows, points, order):
    for r in range(BAND):
        for k in range(2):
            got = rows[r, pl.ds(k * GM + order, BANDS, stride=GK), :]
            points[r * BANDS : (r + 1) * BANDS, k * 128 : (k + 1) * 128] = got.astype(BF16)


def scatter_points(synth, made, order):
    for r in range(BAND):
        for k in range(2):
            made[r, pl.ds(k * GM + order, BANDS, stride=GK), :] = synth[
                r * BANDS : (r + 1) * BANDS, k * 128 : (k + 1) * 128
            ]


def order_factor(order):
    return jnp.where(jnp.logical_or(order == 0, order == LMAX), 1.0, 2.0)


def forward_kernel(
    geo_ref, diag_ref, enc_ref, mix_ref, gain_ref, z_ref, out_ref, leg_out, legt_out,
    table, leg, legt, arrived, rows, points, made, ready, sent_in, got_in, sent_out, got_out, kept
):
    first_order = lax.axis_index("space") * MDEV
    enter()
    for group in range(GROUPS):
        send_group(z_ref, arrived, group, sent_in, got_in)
    legendre_rows(first_order, geo_ref, diag_ref, table)
    legendre_tables(table, leg, legt)
    save = pltpu.make_async_copy(leg, leg_out, kept.at[0])
    save_t = pltpu.make_async_copy(legt, legt_out, kept.at[1])
    save.start()
    save_t.start()
    points[...] = jnp.zeros((PTS, 256), BF16)

    def one_group(group, carry):
        wait_arrived(z_ref, arrived, group, got_in)
        for r in range(BAND):
            base, off = window(r)
            pair = arrived[group, :, :, base : base + 256].astype(F32).reshape(BANDS * GK, 256)
            rows[r] = pltpu.roll(pair, (256 - off) % 256, 1)[:, :128]

        def one_order(order, carry):
            m = group * GM + order
            gather_points(rows, points, order)
            coeffs = dot(leg[m], points[...], 1, 0).astype(BF16)
            gain = gain_ref[...] * order_factor(first_order + m)
            filtered = []
            for k in range(2):
                channels = dot(coeffs[:, k * 128 : (k + 1) * 128], enc_ref[...], 1, 0).astype(BF16)
                filtered.append((dot(channels, mix_ref[...], 1, 0) * gain).astype(BF16))
            scatter_points(dot(legt[m], jnp.concatenate(filtered, axis=1), 1, 0), made, order)
            return carry

        lax.fori_loop(0, GM, one_order, 0)
        for r in range(BAND):
            ready[group, :, :, r * CH : (r + 1) * CH] = (
                made[r].reshape(BANDS, GK, CH).astype(BF16)
            )
        send_group(ready, out_ref, group, sent_out, got_out)
        return carry

    lax.fori_loop(0, GROUPS, one_group, 0)
    save.wait()
    save_t.wait()
    for group in range(GROUPS):
        wait_sent(z_ref, arrived, group, sent_in)
        wait_sent(ready, out_ref, group, sent_out)
        wait_arrived(ready, out_ref, group, got_out)


def backward_kernel(
    enct_ref, mixt_ref, gain_ref, leg_in, legt_in, z_ref, out_ref,
    leg, legt, arrived, rows, points, made, ready, sent_in, got_in, sent_out, got_out, kept
):
    first_order = lax.axis_index("space") * MDEV
    load = pltpu.make_async_copy(leg_in, leg, kept.at[0])
    load_t = pltpu.make_async_copy(legt_in, legt, kept.at[1])
    load.start()
    load_t.start()
    enter()
    for group in range(GROUPS):
        send_group(z_ref, arrived, group, sent_in, got_in)
    points[...] = jnp.zeros((PTS, 256), BF16)
    load.wait()
    load_t.wait()

    def one_group(group, carry):
        wait_arrived(z_ref, arrived, group, got_in)
        for r in range(BAND):
            rows[r] = (
                arrived[group, :, :, r * CH : (r + 1) * CH].astype(F32).reshape(BANDS * GK, CH)
            )

        def one_order(order, carry):
            m = group * GM + order
            gather_points(rows, points, order)
            grads = dot(leg[m], points[...], 1, 0)
            gain = gain_ref[...] * order_factor(first_order + m)
            back = []
            for k in range(2):
                scaled = (grads[:, k * 128 : (k + 1) * 128] * gain).astype(BF16)
                channels = dot(scaled, mixt_ref[...], 1, 0).astype(BF16)
                back.append(dot(channels, enct_ref[...], 1, 0).astype(BF16))
            scatter_points(dot(legt[m], jnp.concatenate(back, axis=1), 1, 0), made, order)
            return carry

        lax.fori_loop(0, GM, one_order, 0)

        def put(at, value):
            ready[group, :, :, at : at + 128] = value.reshape(BANDS, GK, 128).astype(BF16)

        low = spill = jnp.zeros((BANDS * GK, 128), F32)
        at = 0
        for r in range(BAND):
            base, off = window(r)
            while at < base:
                put(at, low)
                low = spill
                at += 128
            value = made[r]
            moved = pltpu.roll(jnp.concatenate([value, jnp.zeros_like(value)], axis=1), off, 1)
            low = low + moved[:, :128]
            spill = moved[:, 128:]
        put(at, low)
        put(at + 128, spill)
        send_group(ready, out_ref, group, sent_out, got_out)
        return carry

    lax.fori_loop(0, GROUPS, one_group, 0)
    for group in range(GROUPS):
        wait_sent(z_ref, arrived, group, sent_in)
        wait_sent(ready, out_ref, group, sent_out)
        wait_arrived(ready, out_ref, group, got_out)


VMEM = pl.BlockSpec(memory_space=pltpu.VMEM)
ANY = pl.BlockSpec(memory_space=pl.ANY)
LEG = jax.ShapeDtypeStruct((MDEV, DEG, PTS), BF16)
LEGT = jax.ShapeDtypeStruct((MDEV, PTS, DEG), BF16)


def chunks(lanes):
    return (GROUPS, BANDS, GK, lanes)


def spectral_scratch(lanes_in, lanes_out):
    return [
        pltpu.VMEM(LEG.shape, BF16),
        pltpu.VMEM(LEGT.shape, BF16),
        pltpu.VMEM(chunks(lanes_in), BF16),
        pltpu.VMEM((BAND, BANDS * GK, 128), F32),
        pltpu.VMEM((PTS, 256), BF16),
        pltpu.VMEM((BAND, BANDS * GK, 128), F32),
        pltpu.VMEM(chunks(lanes_out), BF16),
    ] + [pltpu.SemaphoreType.DMA((GROUPS,))] * 4 + [pltpu.SemaphoreType.DMA((2,))]


def remote_params(collective):
    return pltpu.CompilerParams(
        collective_id=collective, vmem_limit_bytes=58 * 1024 * 1024, has_side_effects=True
    )


def forward(geo, diag, enc, mix, gain, z):
    return pl.pallas_call(
        forward_kernel,
        in_specs=[VMEM] * 6,
        out_specs=[ANY] * 3,
        out_shape=[jax.ShapeDtypeStruct(chunks(WIDE), BF16), LEG, LEGT],
        scratch_shapes=[pltpu.VMEM((PTS // 128, DEG * 16, 128), F32)]
        + spectral_scratch(FLAT, WIDE),
        compiler_params=remote_params(1),
        name="forward",
    )(geo, diag, enc, mix, gain, z)


def backward(enct, mixt, gain, leg, legt, z):
    return pl.pallas_call(
        backward_kernel,
        in_specs=[VMEM] * 3 + [ANY] * 2 + [VMEM],
        out_specs=ANY,
        out_shape=jax.ShapeDtypeStruct(chunks(FLAT), BF16),
        scratch_shapes=spectral_scratch(WIDE, FLAT),
        compiler_params=remote_params(2),
        name="backward",
    )(enct, mixt, gain, leg, legt, z)


TILES = [(t * 128, min(128, NLON - t * 128)) for t in range(6)]


def score_tile(p_ref, o_ref, out_ref, group, lanes, area):
    values = [p_ref[group, e, :, lanes].astype(F32) for e in range(MEMBERS)]
    truth = o_ref[group, :, lanes].astype(F32)

    def inverse(gap):
        return lax.rsqrt(jnp.sum(gap * gap, axis=0, keepdims=True) + EPSILON)

    weights = {}
    for e in range(MEMBERS):
        for f in range(e):
            weights[e, f] = weights[f, e] = inverse(values[e] - values[f]) * (area / MEMBERS)
    for e in range(MEMBERS):
        gap = values[e] - truth
        total = gap * (inverse(gap) * area)
        for f in range(MEMBERS):
            if f != e:
                total = total - (values[e] - values[f]) * weights[e, f]
        out_ref[group, e, :, lanes] = total.astype(BF16)


def middle_kernel(
    live_ref, area_ref, s_ref, c_ref, x_ref, o_ref, enct_ref, dect_ref, dec_ref,
    pred_ref, score_ref, out_ref,
    mine, everyone, share, slope, wide_rows, sent_in, got_in, sent_out, got_out,
):
    band, member = lax.axis_index("space"), lax.axis_index("member")
    barrier = pltpu.get_barrier_semaphore()
    for i in range(1, MEMBERS):
        peer = lax.rem(member + i, MEMBERS)
        pl.semaphore_signal(barrier, inc=1, device_id=(peer, band), device_id_type=MESH)
    pl.semaphore_wait(barrier, MEMBERS - 1)

    def send(source, target, group, peer, sent, got):
        pltpu.make_async_remote_copy(
            src_ref=source.at[group, peer],
            dst_ref=target.at[group, member],
            send_sem=sent.at[group],
            recv_sem=got.at[group],
            device_id=(peer, band),
            device_id_type=MESH,
        ).start()

    def keep(source, target, group, got):
        pltpu.make_async_copy(
            source.at[group, member], target.at[group, member], got.at[group]
        ).start()

    def one_row(group, peer):
        row = 2 * peer + group
        held = jnp.minimum(row, BAND - 1)
        lanes = pl.ds(pl.multiple_of(held * CH, CH), CH)
        field = dot(s_ref[:, lanes], c_ref[...], 0, 0)
        live = live_ref[row]
        state = x_ref[held]
        hidden = (dot(enct_ref[...], state, 1, 0) * live).astype(BF16).astype(F32)
        cdf = 0.5 * (1.0 + lax.erf(field * (1.0 / math.sqrt(2.0))))
        gradient = cdf + field * jnp.exp(-0.5 * field * field) * (1.0 / math.sqrt(2.0 * math.pi))
        block = ((field * cdf + hidden) * live).astype(BF16)
        decoded = dot(dect_ref[...], block, 1, 0)
        result = (state.astype(F32) + decoded) * live
        mine[group, peer] = result.astype(BF16)
        slope[group, peer] = gradient.astype(BF16)
        for t, (start, size) in enumerate(TILES):
            wide_rows[t, pl.ds(row, FIELDS, stride=16), :size] = result[:, start : start + size]

    for group in range(2):

        def one_peer(i, carry):
            peer = lax.rem(member + i, MEMBERS)
            one_row(group, peer)
            send(mine, everyone, group, peer, sent_in, got_in)
            return carry

        lax.fori_loop(1, MEMBERS, one_peer, 0)
        one_row(group, member)
        keep(mine, everyone, group, got_in)

    for t, (start, size) in enumerate(TILES):
        rows = wide_rows[t].reshape(FIELDS, 16, 128)
        pred_ref[:, :, start : start + size] = rows[:, :BAND, :size].astype(BF16)

    def score_group(group, carry):
        pltpu.make_async_copy(mine.at[group], everyone.at[group], got_in.at[group]).wait()
        area = area_ref[2 * member + group]

        def one_tile(t, inner):
            lanes = pl.ds(pl.multiple_of(t * 128, 128), 128)
            score_tile(everyone, o_ref, share, group, lanes, area)
            return inner

        lax.fori_loop(0, 5, one_tile, 0)
        score_tile(everyone, o_ref, share, group, pl.ds(640, NLON - 640), area)

        def one_peer(i, inner):
            send(share, score_ref, group, lax.rem(member + i, MEMBERS), sent_out, got_out)
            return inner

        lax.fori_loop(1, MEMBERS, one_peer, 0)
        keep(share, score_ref, group, got_out)
        return carry

    lax.fori_loop(0, 2, score_group, 0)

    for group in range(2):
        pltpu.make_async_copy(share.at[group], score_ref.at[group], got_out.at[group]).wait()
        for first in range(0, MEMBERS, 2):
            fields = []
            for peer in (first, first + 1):
                block = dot(dec_ref[...], score_ref[group, peer], 1, 0)
                fields.append((block * slope[group, peer].astype(F32)).astype(BF16))
            made = dot(c_ref[...], jnp.concatenate(fields, axis=0), 1, 1).astype(BF16)
            for part in range(2):
                row = 2 * (first + part) + group
                if row < BAND:
                    out_ref[:, row * CH : (row + 1) * CH] = made[:, part * CH : (part + 1) * CH]

    most = pl.ds(0, MEMBERS - 1)
    for group in range(2):
        for source, target, sent in ((mine, everyone, sent_in), (share, score_ref, sent_out)):
            pltpu.make_async_copy(
                source.at[group, most], target.at[group, most], sent.at[group]
            ).wait()


def middle(live, area, s, c, x, truth, enct, dect, dec):
    quarter = (2, MEMBERS, FIELDS, NLON)
    return pl.pallas_call(
        middle_kernel,
        in_specs=[SMEM] * 2 + [VMEM] * 7,
        out_specs=[VMEM] * 3,
        out_shape=[
            jax.ShapeDtypeStruct((FIELDS, BAND, NLON), BF16),
            jax.ShapeDtypeStruct(quarter, BF16),
            jax.ShapeDtypeStruct((BANDS * KM, WIDE), BF16),
        ],
        scratch_shapes=[
            pltpu.VMEM(quarter, BF16),
            pltpu.VMEM(quarter, BF16),
            pltpu.VMEM(quarter, BF16),
            pltpu.VMEM((2, MEMBERS, CH, NLON), BF16),
            pltpu.VMEM((len(TILES), FIELDS * 16, 128), F32),
        ]
        + [pltpu.SemaphoreType.DMA((2,))] * 4,
        compiler_params=remote_params(3),
        name="middle",
    )(live, area, s, c, x, truth, enct, dect, dec)


def final_kernel(weight_ref, live_ref, z_ref, c_ref, g_ref, dec_ref, enc_ref, out_ref, spread):
    spread[...] = dot(z_ref[...], c_ref[...], 0, 0)
    for r in range(BAND):
        score = g_ref[r % 2, r // 2]
        block = dot(dec_ref[...], score, 1, 0).astype(BF16)
        local = dot(enc_ref[...], block, 1, 0)
        far = spread[r * FIELDS : (r + 1) * FIELDS, :] * weight_ref[r]
        out_ref[r] = ((score.astype(F32) + local + far) * live_ref[r]).astype(BF16)


def final_stage(weight, live, z, c, score, dec, enc):
    return pl.pallas_call(
        final_kernel,
        in_specs=[SMEM, SMEM] + [pl.BlockSpec(memory_space=pltpu.VMEM)] * 5,
        out_specs=pl.BlockSpec(memory_space=pltpu.VMEM),
        out_shape=jax.ShapeDtypeStruct((BAND, FIELDS, NLON), BF16),
        scratch_shapes=[pltpu.VMEM((FLAT, NLON), F32)],
        compiler_params=pltpu.CompilerParams(vmem_limit_bytes=56 * 1024 * 1024),
        name="final_stage",
    )(weight, live, z, c, score, dec, enc)


def on_device(
    states, observed, band_rows, encoder_weight, mixing_weight, degree_gain, decoder_weight
):
    band = lax.axis_index("space")
    member = lax.axis_index("member")
    first = band * MDEV

    number = jnp.arange(BANDS, dtype=jnp.int32)
    point = jnp.arange(PTS, dtype=jnp.int32)
    point_band, point_row = point % BANDS, point // BANDS
    starts = jnp.sum(jnp.where(number[:, None] < point_band[None], band_rows[:, None], 0), axis=0)
    counts = jnp.sum(jnp.where(number[:, None] == point_band[None], band_rows[:, None], 0), axis=0)
    colatitude = jnp.minimum(starts + point_row, NLAT - 1).astype(F32) * (math.pi / (NLAT - 1))
    log_sine = jnp.log(jnp.maximum(jnp.sin(colatitude), 1e-30))
    live = (point_row < counts).astype(F32)
    zero = jnp.zeros_like(live)
    geo = jnp.stack([jnp.cos(colatitude), log_sine, live] + [zero] * 5)
    own_start = jnp.sum(jnp.where(number < band, band_rows, 0))
    own_count = jnp.sum(jnp.where(number == band, band_rows, 0))
    row = jnp.arange(16, dtype=jnp.int32)
    own_live = (row < own_count).astype(F32)
    own_lat = jnp.minimum(own_start + row, NLAT - 1).astype(F32) * (math.pi / (NLAT - 1))
    own_sine = jnp.sin(own_lat)
    own_weight = own_live * own_sine * (math.pi / (NLAT - 1) / NLON)
    own_area = 8.0 * own_sine * own_live

    c = fourier_table()
    diag = lax.dynamic_slice_in_dim(jnp.asarray(diagonal_logs()), first, 16)
    diag = jnp.broadcast_to(diag[:, None], (16, 128))
    gain = jnp.pad(degree_gain, ((0, DEG - degree_gain.shape[0]), (0, 0)))
    enc = encoder_weight
    enct = enc.T
    dec = decoder_weight
    dect = dec.T
    enc_wide = jnp.pad(enc, ((0, 128 - FIELDS), (0, 0)))
    enct_wide = enc_wide.T

    x = jnp.transpose(states[0], (1, 0, 2))
    flat = jnp.pad(x.reshape(BAND * FIELDS, NLON), ((0, FLAT - BAND * FIELDS), (0, 0)))
    lane_row = jnp.arange(FLAT, dtype=jnp.int32) // FIELDS
    lane_weight = jnp.sum(jnp.where(row[:, None] == lane_row[None], own_weight[:, None], 0.0), axis=0)
    zonal = (
        jnp.einsum("aj,bj->ab", c, flat, preferred_element_type=F32) * lane_weight[None]
    ).astype(BF16)

    synth, leg, legt = forward(geo, diag, enc_wide, mixing_weight, gain, zonal.reshape(chunks(FLAT)))
    synth = synth.reshape(BANDS * KM, WIDE)
    padded = jnp.pad(observed, ((0, 0), (0, 1), (0, 0)))
    truth = jnp.transpose(lax.dynamic_slice_in_dim(padded, member * 2, 2, 1), (1, 0, 2))
    prediction, score, grads = middle(own_live, own_area, synth, c, x, truth, enct, dect, dec)

    grads = backward(
        enct_wide, mixing_weight.T, gain, leg, legt, grads.reshape(chunks(WIDE))
    )
    grads = grads.reshape(BANDS * KM, FLAT)
    result = final_stage(own_weight, own_live, grads, c, score, dec, enc)
    return (prediction[None], jnp.transpose(result, (1, 0, 2))[None])


def solution(mesh):
    in_specs = (P("member", None, "space", None), P(None, "space", None), P(), P(), P(), P(), P())
    out_specs = (P("member", None, "space", None), P("member", None, "space", None))
    return jax.shard_map(
        on_device, mesh=mesh, in_specs=in_specs, out_specs=out_specs, check_vma=False
    )
```

```python
import math

import jax
import jax.numpy as jnp
import numpy as np
from jax import lax
from jax.experimental import pallas as pl
from jax.experimental.pallas import tpu as pltpu
from jax.sharding import PartitionSpec as P

NLAT = 361
LMAX = 360
NLON = 720
FIELDS = 73
CH = 128
BAND = 15
BANDS = 32
MEMBERS = 8
MDEV = 12
DEG = 384
PTS = 512
KM = 2 * MDEV
GROUPS = 3
GM = MDEV // GROUPS
GK = 2 * GM
MESH = pl.DeviceIdType.MESH
IDLE = (3, 9, 16, 22, 29)
BUSY = BANDS - len(IDLE)
FLAT = 1152
WIDE = BAND * CH

EPSILON = 1e-05
F32 = jnp.float32
BF16 = jnp.bfloat16


def dot(a, b, ca, cb):
    return lax.dot_general(a, b, (((ca,), (cb,)), ((), ())), preferred_element_type=F32)


SMEM = pl.BlockSpec(memory_space=pltpu.SMEM)
VMEM = pl.BlockSpec(memory_space=pltpu.VMEM)
ANY = pl.BlockSpec(memory_space=pl.ANY)
TILES = [(t * 128, min(128, NLON - t * 128)) for t in range(6)]


def group_orders():
    first = np.zeros((GROUPS, BANDS), np.int64)
    first[:2] = np.arange(2 * BANDS).reshape(2, BANDS) * GM
    rank = 2 * BANDS
    for owner in range(BANDS):
        idle = owner in IDLE
        first[2, owner] = (GROUPS * BANDS - 1 if idle else rank) * GM
        rank += 0 if idle else 1
    return first


def is_idle(device):
    found = device == IDLE[0]
    for other in IDLE[1:]:
        found = jnp.logical_or(found, device == other)
    return found


def first_of_group(group, device):
    skipped = sum(jnp.where(device > other, 1, 0) for other in IDLE)
    last = jnp.where(is_idle(device), GROUPS * BANDS - 1, 2 * BANDS + device - skipped)
    return jnp.where(group == 2, last, group * BANDS + device) * GM


def fourier_table():
    orders = group_orders()[:, :, None] + np.arange(GM)
    angle = 2.0 * np.pi * ((orders[..., None] * np.arange(NLON)) % NLON) / NLON
    live = (orders <= LMAX)[..., None]
    both = np.stack([np.where(live, np.cos(angle), 0.0), np.where(live, -np.sin(angle), 0.0)])
    both = both.transpose(1, 2, 0, 3, 4).reshape(BANDS * KM, NLON)
    return jnp.asarray(both.astype(np.float32), BF16)


def diagonal_logs():
    k = np.arange(1, BANDS * MDEV + 16, dtype=np.float64)
    steps = 0.5 * np.log((2.0 * k + 1.0) / (2.0 * k))
    logs = np.concatenate([[0.0], np.cumsum(steps)]).astype(np.float32) + np.float32(
        0.5 * math.log(0.5)
    )
    first = group_orders()
    orders = np.stack([first[0], first[1], first[2], first[2]])[:, :, None] + np.arange(GM)
    orders = orders.transpose(1, 0, 2).reshape(BANDS, 16)
    return np.broadcast_to(logs[orders][:, :, None], (BANDS, 16, 128))


def legendre_rows(geo_ref, diag_ref, table):
    band = lax.axis_index("space")
    cosine = jnp.broadcast_to(geo_ref[0:1, :], (16, PTS))
    log_sine = geo_ref[1:2, :]
    live = jnp.broadcast_to(geo_ref[2:3, :], (16, PTS))
    sublane = lax.broadcasted_iota(jnp.int32, (16, 128), 0)
    orders = jnp.where(
        sublane < GM,
        first_of_group(0, band) + sublane,
        jnp.where(
            sublane < 2 * GM,
            first_of_group(1, band) + sublane - GM,
            first_of_group(2, band) + jnp.bitwise_and(sublane, GM - 1),
        ),
    )
    order_f = orders.astype(F32)
    order_sq = order_f * order_f

    def wide(x):
        return jnp.concatenate([x] * (PTS // 128), axis=1)

    start = wide(diag_ref[...]) + wide(order_f) * log_sine

    def block(number, carry):
        first, second, log_scale = carry
        scale = jnp.exp(log_scale) * live
        for position in range(16):
            degree = number * 16 + position
            lf = jnp.full((16, 128), degree, jnp.int32).astype(F32)
            up = jnp.sqrt((4.0 * lf * lf - 1.0) / jnp.maximum(lf * lf - order_sq, 1.0))
            lb = lf - 1.0
            back = jnp.sqrt(
                jnp.maximum(lb * lb - order_sq, 0.0) / jnp.maximum(4.0 * lb * lb - 1.0, 1.0)
            )
            up = jnp.where(degree > orders, up, 0.0)
            onset = jnp.where(degree == orders, 1.0, 0.0)
            current = wide(up) * (cosine * first - wide(back) * second) + wide(onset)
            kept = jnp.where(jnp.full((16, PTS), degree, jnp.int32) <= LMAX, current * scale, 0.0)
            for part in range(PTS // 128):
                table[part, pl.ds(pl.multiple_of(degree * 16, 16), 16), :] = kept[
                    :, part * 128 : part * 128 + 128
                ]
            second = first
            first = current
        magnitude = jnp.maximum(jnp.abs(first), jnp.abs(second))
        factor = jnp.where(magnitude > 1.0, magnitude, 1.0)
        return first / factor, second / factor, log_scale + jnp.log(factor)

    zero = jnp.zeros((16, PTS), F32)
    lax.fori_loop(0, 23, block, (zero, zero, start))
    table[:, pl.ds(368 * 16, 16 * 16), :] = jnp.zeros((PTS // 128, 256, 128), F32)


def legendre_tables(table, leg, legt):
    def one(m, carry):
        for part in range(PTS // 128):
            lanes = slice(part * 128, part * 128 + 128)
            values = table[part, pl.ds(m, DEG, stride=16), :]
            leg[m, :, lanes] = values.astype(BF16)
            legt[m, lanes, :] = values.T.astype(BF16)
        return carry

    lax.fori_loop(0, MDEV, one, 0)


def window(row):
    start = row * FIELDS
    return start // 128 * 128, start % 128


def enter():
    band, member = lax.axis_index("space"), lax.axis_index("member")
    barrier = pltpu.get_barrier_semaphore()

    def signal(i, carry):
        peer = lax.rem(band + i, BANDS)
        pl.semaphore_signal(barrier, inc=1, device_id=(member, peer), device_id_type=MESH)
        return carry

    lax.fori_loop(1, BANDS, signal, 0)
    pl.semaphore_wait(barrier, BANDS - 1)


def send_in(source, target, group, sent, got):
    band, member = lax.axis_index("space"), lax.axis_index("member")

    def send(i, carry):
        peer = lax.rem(band + i, BANDS)

        def start():
            pltpu.make_async_remote_copy(
                src_ref=source.at[group, peer],
                dst_ref=target.at[group, band],
                send_sem=sent.at[group],
                recv_sem=got.at[group],
                device_id=(member, peer),
                device_id_type=MESH,
            ).start()

        if group == 2:
            pl.when(jnp.logical_not(is_idle(peer)))(start)
        else:
            start()
        return carry

    lax.fori_loop(1, BANDS, send, 0)

    def own():
        pltpu.make_async_copy(
            source.at[group, band], target.at[group, band], got.at[group]
        ).start()

    if group == 2:
        pl.when(jnp.logical_not(is_idle(band)))(own)
    else:
        own()


def send_out(source, target, group, sent, got):
    band, member = lax.axis_index("space"), lax.axis_index("member")

    def send(i, carry):
        peer = lax.rem(band + i, BANDS)
        pltpu.make_async_remote_copy(
            src_ref=source.at[group, peer],
            dst_ref=target.at[group, band],
            send_sem=sent.at[group],
            recv_sem=got.at[group],
            device_id=(member, peer),
            device_id_type=MESH,
        ).start()
        return carry

    lax.fori_loop(1, BANDS, send, 0)
    pltpu.make_async_copy(source.at[group, band], target.at[group, band], got.at[group]).start()


def wait_chunks(array, group, count, sem):
    part = array.at[group, pl.ds(0, count)]
    pltpu.make_async_copy(part, part, sem.at[group]).wait()


def wait_sent(first, second, sent_first, sent_second):
    for group in range(2):
        wait_chunks(first, group, BANDS - 1, sent_first)
        wait_chunks(second, group, BANDS - 1, sent_second)
    idle = is_idle(lax.axis_index("space"))

    @pl.when(idle)
    def _():
        wait_chunks(first, 2, BUSY, sent_first)

    @pl.when(jnp.logical_not(idle))
    def _():
        wait_chunks(first, 2, BUSY - 1, sent_first)
        wait_chunks(second, 2, BANDS - 1, sent_second)


def clear_idle(target):
    for owner in IDLE:
        target[2, owner] = jnp.zeros(target.shape[2:], BF16)


def each_busy_group(work):
    idle = is_idle(lax.axis_index("space"))

    def one_group(group, carry):
        pl.when(jnp.logical_not(jnp.logical_and(group == 2, idle)))(lambda: work(group))
        return carry

    lax.fori_loop(0, GROUPS, one_group, 0)


def gather_points(rows, points, order):
    for r in range(BAND):
        for k in range(2):
            got = rows[r, pl.ds(k * GM + order, BANDS, stride=GK), :]
            points[r * BANDS : (r + 1) * BANDS, k * 128 : (k + 1) * 128] = got.astype(BF16)


def scatter_points(synth, made, order):
    for r in range(BAND):
        for k in range(2):
            made[r, pl.ds(k * GM + order, BANDS, stride=GK), :] = synth[
                r * BANDS : (r + 1) * BANDS, k * 128 : (k + 1) * 128
            ]


def order_factor(order):
    return jnp.where(jnp.logical_or(order == 0, order == LMAX), 1.0, 2.0)


def forward_kernel(
    geo_ref, diag_ref, enc_ref, mix_ref, gain_ref, z_ref, out_ref, leg_out, legt_out,
    table, leg, legt, arrived, rows, points, made, ready, sent_in, got_in, sent_out, got_out, kept
):
    band = lax.axis_index("space")
    enter()
    for group in range(GROUPS):
        send_in(z_ref, arrived, group, sent_in, got_in)
    clear_idle(out_ref)
    legendre_rows(geo_ref, diag_ref, table)
    legendre_tables(table, leg, legt)
    save = pltpu.make_async_copy(leg, leg_out, kept.at[0])
    save_t = pltpu.make_async_copy(legt, legt_out, kept.at[1])
    save.start()
    save_t.start()
    points[...] = jnp.zeros((PTS, 256), BF16)

    def one_group(group):
        wait_chunks(arrived, group, BANDS, got_in)
        first_order = first_of_group(group, band)
        for r in range(BAND):
            base, off = window(r)
            pair = arrived[group, :, :, base : base + 256].astype(F32).reshape(BANDS * GK, 256)
            rows[r] = pltpu.roll(pair, (256 - off) % 256, 1)[:, :128]

        def one_order(order, carry):
            m = group * GM + order
            gather_points(rows, points, order)
            coeffs = dot(leg[m], points[...], 1, 0).astype(BF16)
            gain = padded_gain(gain_ref) * order_factor(first_order + order)
            filtered = []
            for k in range(2):
                channels = dot(coeffs[:, k * 128 : (k + 1) * 128], enc_ref[...], 1, 0).astype(BF16)
                filtered.append((dot(channels, mix_ref[...], 1, 0) * gain).astype(BF16))
            scatter_points(dot(legt[m], jnp.concatenate(filtered, axis=1), 1, 0), made, order)
            return carry

        lax.fori_loop(0, GM, one_order, 0)
        for r in range(BAND):
            ready[group, :, :, r * CH : (r + 1) * CH] = (
                made[r].reshape(BANDS, GK, CH).astype(BF16)
            )
        send_out(ready, out_ref, group, sent_out, got_out)

    each_busy_group(one_group)
    save.wait()
    save_t.wait()
    wait_sent(z_ref, ready, sent_in, sent_out)
    for group in range(GROUPS):
        wait_chunks(out_ref, group, BUSY if group == 2 else BANDS, got_out)


def padded_gain(gain_ref):
    rows = gain_ref.shape[0]
    return jnp.concatenate([gain_ref[...], jnp.zeros((DEG - rows, CH), F32)], axis=0)


def backward_kernel(
    weight_ref, live_ref, enct_ref, mixt_ref, gain_ref, enc_ref, dec_ref, c_ref, g_ref,
    leg_in, legt_in, z_ref, out_ref,
    leg, legt, arrived, rows, points, made, ready, sent_in, got_in, sent_out, got_out, kept,
    returned, spread, local, wide_rows,
):
    band = lax.axis_index("space")
    load = pltpu.make_async_copy(leg_in, leg, kept.at[0])
    load_t = pltpu.make_async_copy(legt_in, legt, kept.at[1])
    load.start()
    load_t.start()
    enter()
    for group in range(GROUPS):
        send_in(z_ref, arrived, group, sent_in, got_in)
    clear_idle(returned)
    points[...] = jnp.zeros((PTS, 256), BF16)
    for r in range(BAND):
        score = g_ref[r % 2, r // 2]
        block = dot(dec_ref[...], score, 1, 0).astype(BF16)
        local[r] = score.astype(F32) + dot(enc_ref[...], block, 1, 0)
    load.wait()
    load_t.wait()

    def one_group(group):
        wait_chunks(arrived, group, BANDS, got_in)
        first_order = first_of_group(group, band)
        for r in range(BAND):
            rows[r] = (
                arrived[group, :, :, r * CH : (r + 1) * CH].astype(F32).reshape(BANDS * GK, CH)
            )

        def one_order(order, carry):
            m = group * GM + order
            gather_points(rows, points, order)
            grads = dot(leg[m], points[...], 1, 0)
            gain = padded_gain(gain_ref) * order_factor(first_order + order)
            back = []
            for k in range(2):
                scaled = (grads[:, k * 128 : (k + 1) * 128] * gain).astype(BF16)
                channels = dot(scaled, mixt_ref[...], 1, 0).astype(BF16)
                back.append(dot(channels, enct_ref[...], 1, 0).astype(BF16))
            scatter_points(dot(legt[m], jnp.concatenate(back, axis=1), 1, 0), made, order)
            return carry

        lax.fori_loop(0, GM, one_order, 0)

        def put(at, value):
            ready[group, :, :, at : at + 128] = value.reshape(BANDS, GK, 128).astype(BF16)

        low = spill = jnp.zeros((BANDS * GK, 128), F32)
        at = 0
        for r in range(BAND):
            base, off = window(r)
            while at < base:
                put(at, low)
                low = spill
                at += 128
            value = made[r]
            moved = pltpu.roll(jnp.concatenate([value, jnp.zeros_like(value)], axis=1), off, 1)
            low = low + moved[:, :128]
            spill = moved[:, 128:]
        put(at, low)
        put(at + 128, spill)
        send_out(ready, returned, group, sent_out, got_out)

    each_busy_group(one_group)
    for group in range(GROUPS):
        wait_chunks(returned, group, BUSY if group == 2 else BANDS, got_out)
        block = returned[group].astype(F32).reshape(BANDS * GK, FLAT).astype(BF16)
        part = dot(block, c_ref[group * BANDS * GK : (group + 1) * BANDS * GK, :], 0, 0)
        spread[...] = part if group == 0 else spread[...] + part
    for r in range(BAND):
        far = spread[r * FIELDS : (r + 1) * FIELDS, :] * weight_ref[r]
        result = (local[r] + far) * live_ref[r]
        for t, (start, size) in enumerate(TILES):
            wide_rows[t, pl.ds(r, FIELDS, stride=16), :size] = result[:, start : start + size]
    for t, (start, size) in enumerate(TILES):
        whole = wide_rows[t].reshape(FIELDS, 16, 128)
        out_ref[:, :, start : start + size] = whole[:, :BAND, :size].astype(BF16)
    wait_sent(z_ref, ready, sent_in, sent_out)


LEG = jax.ShapeDtypeStruct((MDEV, DEG, PTS), BF16)
LEGT = jax.ShapeDtypeStruct((MDEV, PTS, DEG), BF16)


def chunks(lanes):
    return (GROUPS, BANDS, GK, lanes)


def spectral_scratch(lanes_in, lanes_out):
    return [
        pltpu.VMEM(LEG.shape, BF16),
        pltpu.VMEM(LEGT.shape, BF16),
        pltpu.VMEM(chunks(lanes_in), BF16),
        pltpu.VMEM((BAND, BANDS * GK, 128), F32),
        pltpu.VMEM((PTS, 256), BF16),
        pltpu.VMEM((BAND, BANDS * GK, 128), F32),
        pltpu.VMEM(chunks(lanes_out), BF16),
    ] + [pltpu.SemaphoreType.DMA((GROUPS,))] * 4 + [pltpu.SemaphoreType.DMA((2,))]


def remote_params(collective):
    return pltpu.CompilerParams(
        collective_id=collective, vmem_limit_bytes=58 * 1024 * 1024, has_side_effects=True
    )


def forward(geo, diag, enc, mix, gain, z):
    return pl.pallas_call(
        forward_kernel,
        in_specs=[VMEM] * 6,
        out_specs=[VMEM, ANY, ANY],
        out_shape=[jax.ShapeDtypeStruct(chunks(WIDE), BF16), LEG, LEGT],
        scratch_shapes=[pltpu.VMEM((PTS // 128, DEG * 16, 128), F32)]
        + spectral_scratch(FLAT, WIDE),
        compiler_params=remote_params(1),
        name="forward",
    )(geo, diag, enc, mix, gain, z)


def backward(weight, live, enct, mixt, gain, enc, dec, c, score, leg, legt, z):
    return pl.pallas_call(
        backward_kernel,
        in_specs=[SMEM] * 2 + [VMEM] * 7 + [ANY] * 2 + [VMEM],
        out_specs=VMEM,
        out_shape=jax.ShapeDtypeStruct((FIELDS, BAND, NLON), BF16),
        scratch_shapes=spectral_scratch(WIDE, FLAT)
        + [
            pltpu.VMEM(chunks(FLAT), BF16),
            pltpu.VMEM((FLAT, NLON), F32),
            pltpu.VMEM((BAND, FIELDS, NLON), F32),
            pltpu.VMEM((len(TILES), FIELDS * 16, 128), F32),
        ],
        compiler_params=remote_params(2),
        name="backward",
    )(weight, live, enct, mixt, gain, enc, dec, c, score, leg, legt, z)


def score_tile(p_ref, o_ref, out_ref, group, lanes, area):
    values = [p_ref[group, e, :, lanes].astype(F32) for e in range(MEMBERS)]
    truth = o_ref[group, :, lanes].astype(F32)

    def inverse(gap):
        return lax.rsqrt(jnp.sum(gap * gap, axis=0, keepdims=True) + EPSILON)

    weights = {}
    for e in range(MEMBERS):
        for f in range(e):
            weights[e, f] = weights[f, e] = inverse(values[e] - values[f]) * (area / MEMBERS)
    for e in range(MEMBERS):
        gap = values[e] - truth
        total = gap * (inverse(gap) * area)
        for f in range(MEMBERS):
            if f != e:
                total = total - (values[e] - values[f]) * weights[e, f]
        out_ref[group, e, :, lanes] = total.astype(BF16)


def middle_kernel(
    live_ref, area_ref, s_ref, c_ref, x_ref, o_ref, enct_ref, dect_ref, dec_ref,
    pred_ref, score_ref, out_ref,
    mine, everyone, share, slope, wide_rows, sent_in, got_in, sent_out, got_out,
):
    band, member = lax.axis_index("space"), lax.axis_index("member")
    barrier = pltpu.get_barrier_semaphore()
    for i in range(1, MEMBERS):
        peer = lax.rem(member + i, MEMBERS)
        pl.semaphore_signal(barrier, inc=1, device_id=(peer, band), device_id_type=MESH)
    pl.semaphore_wait(barrier, MEMBERS - 1)

    def send(source, target, group, peer, sent, got):
        pltpu.make_async_remote_copy(
            src_ref=source.at[group, peer],
            dst_ref=target.at[group, member],
            send_sem=sent.at[group],
            recv_sem=got.at[group],
            device_id=(peer, band),
            device_id_type=MESH,
        ).start()

    def keep(source, target, group, got):
        pltpu.make_async_copy(
            source.at[group, member], target.at[group, member], got.at[group]
        ).start()

    def one_row(group, peer):
        row = 2 * peer + group
        held = jnp.minimum(row, BAND - 1)
        lanes = pl.ds(pl.multiple_of(held * CH, CH), CH)
        field = dot(s_ref[:, lanes], c_ref[...], 0, 0)
        live = live_ref[row]
        state = x_ref[held]
        hidden = (dot(enct_ref[...], state, 1, 0) * live).astype(BF16).astype(F32)
        cdf = 0.5 * (1.0 + lax.erf(field * (1.0 / math.sqrt(2.0))))
        gradient = cdf + field * jnp.exp(-0.5 * field * field) * (1.0 / math.sqrt(2.0 * math.pi))
        block = ((field * cdf + hidden) * live).astype(BF16)
        decoded = dot(dect_ref[...], block, 1, 0)
        result = (state.astype(F32) + decoded) * live
        mine[group, peer] = result.astype(BF16)
        slope[group, peer] = gradient.astype(BF16)
        for t, (start, size) in enumerate(TILES):
            wide_rows[t, pl.ds(row, FIELDS, stride=16), :size] = result[:, start : start + size]

    for group in range(2):

        def one_peer(i, carry):
            peer = lax.rem(member + i, MEMBERS)
            one_row(group, peer)
            send(mine, everyone, group, peer, sent_in, got_in)
            return carry

        lax.fori_loop(1, MEMBERS, one_peer, 0)
        one_row(group, member)
        keep(mine, everyone, group, got_in)

    for t, (start, size) in enumerate(TILES):
        rows = wide_rows[t].reshape(FIELDS, 16, 128)
        pred_ref[:, :, start : start + size] = rows[:, :BAND, :size].astype(BF16)

    def score_group(group, carry):
        pltpu.make_async_copy(mine.at[group], everyone.at[group], got_in.at[group]).wait()
        area = area_ref[2 * member + group]

        def one_tile(t, inner):
            lanes = pl.ds(pl.multiple_of(t * 128, 128), 128)
            score_tile(everyone, o_ref, share, group, lanes, area)
            return inner

        lax.fori_loop(0, 5, one_tile, 0)
        score_tile(everyone, o_ref, share, group, pl.ds(640, NLON - 640), area)

        def one_peer(i, inner):
            send(share, score_ref, group, lax.rem(member + i, MEMBERS), sent_out, got_out)
            return inner

        lax.fori_loop(1, MEMBERS, one_peer, 0)
        keep(share, score_ref, group, got_out)
        return carry

    lax.fori_loop(0, 2, score_group, 0)

    for group in range(2):
        pltpu.make_async_copy(share.at[group], score_ref.at[group], got_out.at[group]).wait()
        for first in range(0, MEMBERS, 2):
            fields = []
            for peer in (first, first + 1):
                block = dot(dec_ref[...], score_ref[group, peer], 1, 0)
                fields.append((block * slope[group, peer].astype(F32)).astype(BF16))
            made = dot(c_ref[...], jnp.concatenate(fields, axis=0), 1, 1).astype(BF16)
            for part in range(2):
                row = 2 * (first + part) + group
                if row < BAND:
                    out_ref[:, row * CH : (row + 1) * CH] = made[:, part * CH : (part + 1) * CH]

    most = pl.ds(0, MEMBERS - 1)
    for group in range(2):
        for source, target, sent in ((mine, everyone, sent_in), (share, score_ref, sent_out)):
            pltpu.make_async_copy(
                source.at[group, most], target.at[group, most], sent.at[group]
            ).wait()


def middle(live, area, s, c, x, truth, enct, dect, dec):
    quarter = (2, MEMBERS, FIELDS, NLON)
    return pl.pallas_call(
        middle_kernel,
        in_specs=[SMEM] * 2 + [VMEM] * 7,
        out_specs=[VMEM] * 3,
        out_shape=[
            jax.ShapeDtypeStruct((FIELDS, BAND, NLON), BF16),
            jax.ShapeDtypeStruct(quarter, BF16),
            jax.ShapeDtypeStruct((BANDS * KM, WIDE), BF16),
        ],
        scratch_shapes=[
            pltpu.VMEM(quarter, BF16),
            pltpu.VMEM(quarter, BF16),
            pltpu.VMEM(quarter, BF16),
            pltpu.VMEM((2, MEMBERS, CH, NLON), BF16),
            pltpu.VMEM((len(TILES), FIELDS * 16, 128), F32),
        ]
        + [pltpu.SemaphoreType.DMA((2,))] * 4,
        compiler_params=remote_params(3),
        name="middle",
    )(live, area, s, c, x, truth, enct, dect, dec)


def on_device(
    states, observed, band_rows, encoder_weight, mixing_weight, degree_gain, decoder_weight
):
    band = lax.axis_index("space")
    member = lax.axis_index("member")

    number = jnp.arange(BANDS, dtype=jnp.int32)
    point = jnp.arange(PTS, dtype=jnp.int32)
    point_band, point_row = point % BANDS, point // BANDS
    starts = jnp.sum(jnp.where(number[:, None] < point_band[None], band_rows[:, None], 0), axis=0)
    counts = jnp.sum(jnp.where(number[:, None] == point_band[None], band_rows[:, None], 0), axis=0)
    colatitude = jnp.minimum(starts + point_row, NLAT - 1).astype(F32) * (math.pi / (NLAT - 1))
    log_sine = jnp.log(jnp.maximum(jnp.sin(colatitude), 1e-30))
    live = (point_row < counts).astype(F32)
    zero = jnp.zeros_like(live)
    geo = jnp.stack([jnp.cos(colatitude), log_sine, live] + [zero] * 5)
    own_start = jnp.sum(jnp.where(number < band, band_rows, 0))
    own_count = jnp.sum(jnp.where(number == band, band_rows, 0))
    row = jnp.arange(16, dtype=jnp.int32)
    own_live = (row < own_count).astype(F32)
    own_lat = jnp.minimum(own_start + row, NLAT - 1).astype(F32) * (math.pi / (NLAT - 1))
    own_sine = jnp.sin(own_lat)
    own_weight = own_live * own_sine * (math.pi / (NLAT - 1) / NLON)
    own_area = 8.0 * own_sine * own_live

    c = fourier_table()
    diag = lax.dynamic_index_in_dim(jnp.asarray(diagonal_logs()), band, 0, keepdims=False)
    enc = encoder_weight
    enct = enc.T
    dec = decoder_weight
    dect = dec.T
    enc_wide = jnp.pad(enc, ((0, 128 - FIELDS), (0, 0)))
    enct_wide = enc_wide.T

    x = jnp.transpose(states[0], (1, 0, 2))
    flat = jnp.pad(x.reshape(BAND * FIELDS, NLON), ((0, FLAT - BAND * FIELDS), (0, 0)))
    lane_row = jnp.arange(FLAT, dtype=jnp.int32) // FIELDS
    lane_weight = jnp.sum(jnp.where(row[:, None] == lane_row[None], own_weight[:, None], 0.0), axis=0)
    zonal = (
        jnp.einsum("aj,bj->ab", c, flat, preferred_element_type=F32) * lane_weight[None]
    ).astype(BF16)

    synth, leg, legt = forward(
        geo, diag, enc_wide, mixing_weight, degree_gain, zonal.reshape(chunks(FLAT))
    )
    synth = synth.reshape(BANDS * KM, WIDE)
    padded = jnp.pad(observed, ((0, 0), (0, 1), (0, 0)))
    truth = jnp.transpose(lax.dynamic_slice_in_dim(padded, member * 2, 2, 1), (1, 0, 2))
    prediction, score, grads = middle(own_live, own_area, synth, c, x, truth, enct, dect, dec)

    result = backward(
        own_weight, own_live, enct_wide, mixing_weight.T, degree_gain, enc, dec, c, score,
        leg, legt, grads.reshape(chunks(WIDE)),
    )
    return (prediction[None], result[None])


def solution(mesh):
    in_specs = (P("member", None, "space", None), P(None, "space", None), P(), P(), P(), P(), P())
    out_specs = (P("member", None, "space", None), P("member", None, "space", None))
    return jax.shard_map(
        on_device, mesh=mesh, in_specs=in_specs, out_specs=out_specs, check_vma=False
    )
```

```python
import math

import jax
import jax.numpy as jnp
import numpy as np
from jax import lax
from jax.experimental import pallas as pl
from jax.experimental.pallas import tpu as pltpu
from jax.sharding import PartitionSpec as P

NLAT = 361
LMAX = 360
NLON = 720
FIELDS = 73
CH = 128
BAND = 15
BANDS = 32
MEMBERS = 8
MDEV = 12
DEG = 384
PTS = 512
KM = 2 * MDEV
GROUPS = 3
GM = MDEV // GROUPS
GK = 2 * GM
MESH = pl.DeviceIdType.MESH
IDLE = (3, 9, 16, 22, 29)
BUSY = BANDS - len(IDLE)
FLAT = 1152
WIDE = BAND * CH

EPSILON = 1e-05
F32 = jnp.float32
BF16 = jnp.bfloat16


def dot(a, b, ca, cb):
    return lax.dot_general(a, b, (((ca,), (cb,)), ((), ())), preferred_element_type=F32)


SMEM = pl.BlockSpec(memory_space=pltpu.SMEM)
VMEM = pl.BlockSpec(memory_space=pltpu.VMEM)
ANY = pl.BlockSpec(memory_space=pl.ANY)
TILES = [(t * 128, min(128, NLON - t * 128)) for t in range(6)]


def group_orders():
    first = np.zeros((GROUPS, BANDS), np.int64)
    first[:2] = np.arange(2 * BANDS).reshape(2, BANDS) * GM
    rank = 2 * BANDS
    for owner in range(BANDS):
        idle = owner in IDLE
        first[2, owner] = (GROUPS * BANDS - 1 if idle else rank) * GM
        rank += 0 if idle else 1
    return first


def is_idle(device):
    found = device == IDLE[0]
    for other in IDLE[1:]:
        found = jnp.logical_or(found, device == other)
    return found


def first_of_group(group, device):
    skipped = sum(jnp.where(device > other, 1, 0) for other in IDLE)
    last = jnp.where(is_idle(device), GROUPS * BANDS - 1, 2 * BANDS + device - skipped)
    return jnp.where(group == 2, last, group * BANDS + device) * GM


def fourier_table():
    orders = group_orders()[:, :, None] + np.arange(GM)
    angle = 2.0 * np.pi * ((orders[..., None] * np.arange(NLON)) % NLON) / NLON
    live = (orders <= LMAX)[..., None]
    both = np.stack([np.where(live, np.cos(angle), 0.0), np.where(live, -np.sin(angle), 0.0)])
    both = both.transpose(1, 2, 0, 3, 4).reshape(BANDS * KM, NLON)
    return jnp.asarray(both.astype(np.float32), BF16)


def diagonal_logs():
    k = np.arange(1, BANDS * MDEV + 16, dtype=np.float64)
    steps = 0.5 * np.log((2.0 * k + 1.0) / (2.0 * k))
    logs = np.concatenate([[0.0], np.cumsum(steps)]).astype(np.float32) + np.float32(
        0.5 * math.log(0.5)
    )
    first = group_orders()
    orders = np.stack([first[0], first[1], first[2], first[2]])[:, :, None] + np.arange(GM)
    orders = orders.transpose(1, 0, 2).reshape(BANDS, 16)
    return np.broadcast_to(logs[orders][:, :, None], (BANDS, 16, 128))


def legendre_rows(geo_ref, diag_ref, table):
    band = lax.axis_index("space")
    cosine = jnp.broadcast_to(geo_ref[0:1, :], (16, PTS))
    log_sine = geo_ref[1:2, :]
    live = jnp.broadcast_to(geo_ref[2:3, :], (16, PTS))
    sublane = lax.broadcasted_iota(jnp.int32, (16, 128), 0)
    orders = jnp.where(
        sublane < GM,
        first_of_group(0, band) + sublane,
        jnp.where(
            sublane < 2 * GM,
            first_of_group(1, band) + sublane - GM,
            first_of_group(2, band) + jnp.bitwise_and(sublane, GM - 1),
        ),
    )
    order_f = orders.astype(F32)
    order_sq = order_f * order_f

    def wide(x):
        return jnp.concatenate([x] * (PTS // 128), axis=1)

    start = wide(diag_ref[...]) + wide(order_f) * log_sine

    def block(number, carry):
        first, second, log_scale = carry
        scale = jnp.exp(log_scale) * live
        for position in range(16):
            degree = number * 16 + position
            lf = jnp.full((16, 128), degree, jnp.int32).astype(F32)
            up = jnp.sqrt((4.0 * lf * lf - 1.0) / jnp.maximum(lf * lf - order_sq, 1.0))
            lb = lf - 1.0
            back = jnp.sqrt(
                jnp.maximum(lb * lb - order_sq, 0.0) / jnp.maximum(4.0 * lb * lb - 1.0, 1.0)
            )
            up = jnp.where(degree > orders, up, 0.0)
            onset = jnp.where(degree == orders, 1.0, 0.0)
            current = wide(up) * (cosine * first - wide(back) * second) + wide(onset)
            kept = jnp.where(jnp.full((16, PTS), degree, jnp.int32) <= LMAX, current * scale, 0.0)
            for part in range(PTS // 128):
                table[part, pl.ds(pl.multiple_of(degree * 16, 16), 16), :] = kept[
                    :, part * 128 : part * 128 + 128
                ]
            second = first
            first = current
        magnitude = jnp.maximum(jnp.abs(first), jnp.abs(second))
        factor = jnp.where(magnitude > 1.0, magnitude, 1.0)
        return first / factor, second / factor, log_scale + jnp.log(factor)

    zero = jnp.zeros((16, PTS), F32)
    lax.fori_loop(0, 23, block, (zero, zero, start))
    table[:, pl.ds(368 * 16, 16 * 16), :] = jnp.zeros((PTS // 128, 256, 128), F32)


def legendre_tables(table, leg, legt):
    def one(m, carry):
        for part in range(PTS // 128):
            lanes = slice(part * 128, part * 128 + 128)
            values = table[part, pl.ds(m, DEG, stride=16), :]
            leg[m, :, lanes] = values.astype(BF16)
            legt[m, lanes, :] = values.T.astype(BF16)
        return carry

    lax.fori_loop(0, MDEV, one, 0)


def window(row):
    start = row * FIELDS
    return start // 128 * 128, start % 128


def pack_windows(rows, value_of, put):
    low = spill = jnp.zeros((rows, 128), F32)
    at = 0
    for r in range(BAND):
        base, off = window(r)
        while at < base:
            put(at, low)
            low = spill
            at += 128
        value = value_of(r)
        moved = pltpu.roll(jnp.concatenate([value, jnp.zeros_like(value)], axis=1), off, 1)
        low = low + moved[:, :128]
        spill = moved[:, 128:]
    put(at, low)
    put(at + 128, spill)


def announce():
    band, member = lax.axis_index("space"), lax.axis_index("member")
    barrier = pltpu.get_barrier_semaphore()

    def signal(i, carry):
        peer = lax.rem(band + i, BANDS)
        pl.semaphore_signal(barrier, inc=1, device_id=(member, peer), device_id_type=MESH)
        return carry

    lax.fori_loop(1, BANDS, signal, 0)


def enter():
    pl.semaphore_wait(pltpu.get_barrier_semaphore(), BANDS - 1)


def send_in(source, target, group, sent, got):
    band, member = lax.axis_index("space"), lax.axis_index("member")

    def send(i, carry):
        peer = lax.rem(band + i, BANDS)

        def start():
            pltpu.make_async_remote_copy(
                src_ref=source.at[group, peer],
                dst_ref=target.at[group, band],
                send_sem=sent.at[group],
                recv_sem=got.at[group],
                device_id=(member, peer),
                device_id_type=MESH,
            ).start()

        if group == 2:
            pl.when(jnp.logical_not(is_idle(peer)))(start)
        else:
            start()
        return carry

    lax.fori_loop(1, BANDS, send, 0)

    def own():
        pltpu.make_async_copy(
            source.at[group, band], target.at[group, band], got.at[group]
        ).start()

    if group == 2:
        pl.when(jnp.logical_not(is_idle(band)))(own)
    else:
        own()


def send_out(source, target, group, sent, got):
    band, member = lax.axis_index("space"), lax.axis_index("member")

    def send(i, carry):
        peer = lax.rem(band + i, BANDS)
        pltpu.make_async_remote_copy(
            src_ref=source.at[group, peer],
            dst_ref=target.at[group, band],
            send_sem=sent.at[group],
            recv_sem=got.at[group],
            device_id=(member, peer),
            device_id_type=MESH,
        ).start()
        return carry

    lax.fori_loop(1, BANDS, send, 0)
    pltpu.make_async_copy(source.at[group, band], target.at[group, band], got.at[group]).start()


def wait_chunks(array, group, count, sem):
    part = array.at[group, pl.ds(0, count)]
    pltpu.make_async_copy(part, part, sem.at[group]).wait()


def wait_sent(first, second, sent_first, sent_second):
    for group in range(2):
        wait_chunks(first, group, BANDS - 1, sent_first)
        wait_chunks(second, group, BANDS - 1, sent_second)
    idle = is_idle(lax.axis_index("space"))

    @pl.when(idle)
    def _():
        wait_chunks(first, 2, BUSY, sent_first)

    @pl.when(jnp.logical_not(idle))
    def _():
        wait_chunks(first, 2, BUSY - 1, sent_first)
        wait_chunks(second, 2, BANDS - 1, sent_second)


def clear_idle(target):
    for owner in IDLE:
        target[2, owner] = jnp.zeros(target.shape[2:], BF16)


def each_busy_group(work):
    idle = is_idle(lax.axis_index("space"))

    def one_group(group, carry):
        pl.when(jnp.logical_not(jnp.logical_and(group == 2, idle)))(lambda: work(group))
        return carry

    lax.fori_loop(0, GROUPS, one_group, 0)


def gather_points(rows, points, order):
    for r in range(BAND):
        for k in range(2):
            got = rows[r, pl.ds(k * GM + order, BANDS, stride=GK), :]
            points[r * BANDS : (r + 1) * BANDS, k * 128 : (k + 1) * 128] = got.astype(BF16)


def scatter_points(synth, made, order):
    for r in range(BAND):
        for k in range(2):
            made[r, pl.ds(k * GM + order, BANDS, stride=GK), :] = synth[
                r * BANDS : (r + 1) * BANDS, k * 128 : (k + 1) * 128
            ]


def order_factor(order):
    return jnp.where(jnp.logical_or(order == 0, order == LMAX), 1.0, 2.0)


def forward_kernel(
    weight_ref, geo_ref, diag_ref, enc_ref, mix_ref, gain_ref, c_ref, x_ref,
    out_ref, leg_out, legt_out, z_ref, padded,
    table, leg, legt, arrived, rows, points, made, ready, sent_in, got_in, sent_out, got_out, kept
):
    band = lax.axis_index("space")
    announce()
    padded[...] = jnp.zeros(padded.shape, F32)
    for group in range(GROUPS):
        waves = c_ref[group * BANDS * GK : (group + 1) * BANDS * GK, :]

        def zonal(r):
            padded[:, :FIELDS] = dot(waves, x_ref[r], 1, 1) * weight_ref[r]
            return padded[...]

        def put_zonal(at, value):
            z_ref[group, :, :, at : at + 128] = value.reshape(BANDS, GK, 128).astype(BF16)

        pack_windows(BANDS * GK, zonal, put_zonal)
        if group == 0:
            enter()
        send_in(z_ref, arrived, group, sent_in, got_in)
    clear_idle(out_ref)
    legendre_rows(geo_ref, diag_ref, table)
    legendre_tables(table, leg, legt)
    save = pltpu.make_async_copy(leg, leg_out, kept.at[0])
    save_t = pltpu.make_async_copy(legt, legt_out, kept.at[1])
    save.start()
    save_t.start()
    points[...] = jnp.zeros((PTS, 256), BF16)

    def one_group(group):
        wait_chunks(arrived, group, BANDS, got_in)
        first_order = first_of_group(group, band)
        for r in range(BAND):
            base, off = window(r)
            pair = arrived[group, :, :, base : base + 256].astype(F32).reshape(BANDS * GK, 256)
            rows[r] = pltpu.roll(pair, (256 - off) % 256, 1)[:, :128]

        def one_order(order, carry):
            m = group * GM + order
            gather_points(rows, points, order)
            coeffs = dot(leg[m], points[...], 1, 0).astype(BF16)
            gain = padded_gain(gain_ref) * order_factor(first_order + order)
            filtered = []
            for k in range(2):
                channels = dot(coeffs[:, k * 128 : (k + 1) * 128], enc_ref[...], 1, 0).astype(BF16)
                filtered.append((dot(channels, mix_ref[...], 1, 0) * gain).astype(BF16))
            scatter_points(dot(legt[m], jnp.concatenate(filtered, axis=1), 1, 0), made, order)
            return carry

        lax.fori_loop(0, GM, one_order, 0)
        for r in range(BAND):
            ready[group, :, :, r * CH : (r + 1) * CH] = (
                made[r].reshape(BANDS, GK, CH).astype(BF16)
            )
        send_out(ready, out_ref, group, sent_out, got_out)

    each_busy_group(one_group)
    save.wait()
    save_t.wait()
    wait_sent(z_ref, ready, sent_in, sent_out)
    for group in range(GROUPS):
        wait_chunks(out_ref, group, BUSY if group == 2 else BANDS, got_out)


def padded_gain(gain_ref):
    rows = gain_ref.shape[0]
    return jnp.concatenate([gain_ref[...], jnp.zeros((DEG - rows, CH), F32)], axis=0)


def backward_kernel(
    weight_ref, live_ref, enct_ref, mixt_ref, gain_ref, enc_ref, dec_ref, c_ref, g_ref,
    leg_in, legt_in, z_ref, out_ref,
    leg, legt, arrived, rows, points, made, ready, sent_in, got_in, sent_out, got_out, kept,
    returned, spread, local, wide_rows, final, stored,
):
    band = lax.axis_index("space")
    load = pltpu.make_async_copy(leg_in, leg, kept.at[0])
    load_t = pltpu.make_async_copy(legt_in, legt, kept.at[1])
    load.start()
    load_t.start()
    announce()
    enter()
    for group in range(GROUPS):
        send_in(z_ref, arrived, group, sent_in, got_in)
    clear_idle(returned)
    points[...] = jnp.zeros((PTS, 256), BF16)
    for r in range(BAND):
        score = g_ref[r % 2, r // 2]
        block = dot(dec_ref[...], score, 1, 0).astype(BF16)
        local[r] = score.astype(F32) + dot(enc_ref[...], block, 1, 0)
    load.wait()
    load_t.wait()

    def one_group(group):
        wait_chunks(arrived, group, BANDS, got_in)
        first_order = first_of_group(group, band)
        for r in range(BAND):
            rows[r] = (
                arrived[group, :, :, r * CH : (r + 1) * CH].astype(F32).reshape(BANDS * GK, CH)
            )

        def one_order(order, carry):
            m = group * GM + order
            gather_points(rows, points, order)
            grads = dot(leg[m], points[...], 1, 0)
            gain = padded_gain(gain_ref) * order_factor(first_order + order)
            back = []
            for k in range(2):
                scaled = (grads[:, k * 128 : (k + 1) * 128] * gain).astype(BF16)
                channels = dot(scaled, mixt_ref[...], 1, 0).astype(BF16)
                back.append(dot(channels, enct_ref[...], 1, 0).astype(BF16))
            scatter_points(dot(legt[m], jnp.concatenate(back, axis=1), 1, 0), made, order)
            return carry

        lax.fori_loop(0, GM, one_order, 0)

        def put(at, value):
            ready[group, :, :, at : at + 128] = value.reshape(BANDS, GK, 128).astype(BF16)

        pack_windows(BANDS * GK, lambda r: made[r], put)
        send_out(ready, returned, group, sent_out, got_out)

    each_busy_group(one_group)
    for group in range(GROUPS):
        wait_chunks(returned, group, BUSY if group == 2 else BANDS, got_out)
        block = returned[group].astype(F32).reshape(BANDS * GK, FLAT).astype(BF16)
        part = dot(block, c_ref[group * BANDS * GK : (group + 1) * BANDS * GK, :], 0, 0)
        spread[...] = part if group == 0 else spread[...] + part
    for r in range(BAND):
        far = spread[r * FIELDS : (r + 1) * FIELDS, :] * weight_ref[r]
        result = (local[r] + far) * live_ref[r]
        for t, (start, size) in enumerate(TILES):
            wide_rows[t, pl.ds(r, FIELDS, stride=16), :size] = result[:, start : start + size]
    copies = []
    for part, (low, high) in enumerate(((0, 40), (40, FIELDS))):
        for t, (start, size) in enumerate(TILES):
            held = wide_rows[t, low * 16 : high * 16, :].reshape(high - low, 16, 128)
            final[low:high, :, start : start + size] = held[:, :BAND, :size].astype(BF16)
        copies.append(
            pltpu.make_async_copy(
                final.at[pl.ds(low, high - low)], out_ref.at[0, pl.ds(low, high - low)],
                stored.at[part],
            )
        )
        copies[-1].start()
    wait_sent(z_ref, ready, sent_in, sent_out)
    for copy in copies:
        copy.wait()


LEG = jax.ShapeDtypeStruct((MDEV, DEG, PTS), BF16)
LEGT = jax.ShapeDtypeStruct((MDEV, PTS, DEG), BF16)


def chunks(lanes):
    return (GROUPS, BANDS, GK, lanes)


def spectral_scratch(lanes_in, lanes_out):
    return [
        pltpu.VMEM(LEG.shape, BF16),
        pltpu.VMEM(LEGT.shape, BF16),
        pltpu.VMEM(chunks(lanes_in), BF16),
        pltpu.VMEM((BAND, BANDS * GK, 128), F32),
        pltpu.VMEM((PTS, 256), BF16),
        pltpu.VMEM((BAND, BANDS * GK, 128), F32),
        pltpu.VMEM(chunks(lanes_out), BF16),
    ] + [pltpu.SemaphoreType.DMA((GROUPS,))] * 4 + [pltpu.SemaphoreType.DMA((2,))]


def remote_params(collective):
    return pltpu.CompilerParams(
        collective_id=collective, vmem_limit_bytes=58 * 1024 * 1024, has_side_effects=True
    )


def forward(weight, geo, diag, enc, mix, gain, c, x):
    return pl.pallas_call(
        forward_kernel,
        in_specs=[SMEM] + [VMEM] * 7,
        out_specs=[VMEM, ANY, ANY],
        out_shape=[jax.ShapeDtypeStruct(chunks(WIDE), BF16), LEG, LEGT],
        scratch_shapes=[
            pltpu.VMEM(chunks(FLAT), BF16),
            pltpu.VMEM((BANDS * GK, 128), F32),
            pltpu.VMEM((PTS // 128, DEG * 16, 128), F32),
        ]
        + spectral_scratch(FLAT, WIDE),
        compiler_params=remote_params(1),
        name="forward",
    )(weight, geo, diag, enc, mix, gain, c, x)


def backward(weight, live, enct, mixt, gain, enc, dec, c, score, leg, legt, z):
    return pl.pallas_call(
        backward_kernel,
        in_specs=[SMEM] * 2 + [VMEM] * 7 + [ANY] * 2 + [VMEM],
        out_specs=ANY,
        out_shape=jax.ShapeDtypeStruct((1, FIELDS, BAND, NLON), BF16),
        scratch_shapes=spectral_scratch(WIDE, FLAT)
        + [
            pltpu.VMEM(chunks(FLAT), BF16),
            pltpu.VMEM((FLAT, NLON), F32),
            pltpu.VMEM((BAND, FIELDS, NLON), F32),
            pltpu.VMEM((len(TILES), FIELDS * 16, 128), F32),
            pltpu.VMEM((FIELDS, BAND, NLON), BF16),
            pltpu.SemaphoreType.DMA((2,)),
        ],
        compiler_params=remote_params(2),
        name="backward",
    )(weight, live, enct, mixt, gain, enc, dec, c, score, leg, legt, z)


def score_tile(p_ref, o_ref, out_ref, group, lanes, area):
    values = [p_ref[group, e, :, lanes].astype(F32) for e in range(MEMBERS)]
    truth = o_ref[group, :, lanes].astype(F32)

    def inverse(gap):
        return lax.rsqrt(jnp.sum(gap * gap, axis=0, keepdims=True) + EPSILON)

    weights = {}
    for e in range(MEMBERS):
        for f in range(e):
            weights[e, f] = weights[f, e] = inverse(values[e] - values[f]) * (area / MEMBERS)
    for e in range(MEMBERS):
        gap = values[e] - truth
        total = gap * (inverse(gap) * area)
        for f in range(MEMBERS):
            if f != e:
                total = total - (values[e] - values[f]) * weights[e, f]
        out_ref[group, e, :, lanes] = total.astype(BF16)


def middle_kernel(
    live_ref, area_ref, s_ref, c_ref, x_ref, o_ref, enct_ref, dect_ref, dec_ref,
    pred_ref, score_ref, out_ref,
    mine, everyone, share, slope, wide_rows, final, stored, sent_in, got_in, sent_out, got_out,
):
    band, member = lax.axis_index("space"), lax.axis_index("member")
    barrier = pltpu.get_barrier_semaphore()
    for i in range(1, MEMBERS):
        peer = lax.rem(member + i, MEMBERS)
        pl.semaphore_signal(barrier, inc=1, device_id=(peer, band), device_id_type=MESH)
    pl.semaphore_wait(barrier, MEMBERS - 1)

    def send(source, target, group, peer, sent, got):
        pltpu.make_async_remote_copy(
            src_ref=source.at[group, peer],
            dst_ref=target.at[group, member],
            send_sem=sent.at[group],
            recv_sem=got.at[group],
            device_id=(peer, band),
            device_id_type=MESH,
        ).start()

    def keep(source, target, group, got):
        pltpu.make_async_copy(
            source.at[group, member], target.at[group, member], got.at[group]
        ).start()

    def one_row(group, peer):
        row = 2 * peer + group
        held = jnp.minimum(row, BAND - 1)
        lanes = pl.ds(pl.multiple_of(held * CH, CH), CH)
        field = dot(s_ref[:, lanes], c_ref[...], 0, 0)
        live = live_ref[row]
        state = x_ref[held]
        hidden = (dot(enct_ref[...], state, 1, 0) * live).astype(BF16).astype(F32)
        cdf = 0.5 * (1.0 + lax.erf(field * (1.0 / math.sqrt(2.0))))
        gradient = cdf + field * jnp.exp(-0.5 * field * field) * (1.0 / math.sqrt(2.0 * math.pi))
        block = ((field * cdf + hidden) * live).astype(BF16)
        decoded = dot(dect_ref[...], block, 1, 0)
        result = (state.astype(F32) + decoded) * live
        mine[group, peer] = result.astype(BF16)
        slope[group, peer] = gradient.astype(BF16)
        for t, (start, size) in enumerate(TILES):
            wide_rows[t, pl.ds(row, FIELDS, stride=16), :size] = result[:, start : start + size]

    for group in range(2):

        def one_peer(i, carry):
            peer = lax.rem(member + i, MEMBERS)
            one_row(group, peer)
            send(mine, everyone, group, peer, sent_in, got_in)
            return carry

        lax.fori_loop(1, MEMBERS, one_peer, 0)
        one_row(group, member)
        keep(mine, everyone, group, got_in)

    for t, (start, size) in enumerate(TILES):
        held = wide_rows[t].reshape(FIELDS, 16, 128)
        final[:, :, start : start + size] = held[:, :BAND, :size].astype(BF16)
    store = pltpu.make_async_copy(final, pred_ref.at[0], stored.at[0])
    store.start()

    def score_group(group, carry):
        pltpu.make_async_copy(mine.at[group], everyone.at[group], got_in.at[group]).wait()
        area = area_ref[2 * member + group]

        def one_tile(t, inner):
            lanes = pl.ds(pl.multiple_of(t * 128, 128), 128)
            score_tile(everyone, o_ref, share, group, lanes, area)
            return inner

        lax.fori_loop(0, 5, one_tile, 0)
        score_tile(everyone, o_ref, share, group, pl.ds(640, NLON - 640), area)

        def one_peer(i, inner):
            send(share, score_ref, group, lax.rem(member + i, MEMBERS), sent_out, got_out)
            return inner

        lax.fori_loop(1, MEMBERS, one_peer, 0)
        keep(share, score_ref, group, got_out)
        return carry

    lax.fori_loop(0, 2, score_group, 0)

    for group in range(2):
        pltpu.make_async_copy(share.at[group], score_ref.at[group], got_out.at[group]).wait()
        for first in range(0, MEMBERS, 2):
            fields = []
            for peer in (first, first + 1):
                block = dot(dec_ref[...], score_ref[group, peer], 1, 0)
                fields.append((block * slope[group, peer].astype(F32)).astype(BF16))
            made = dot(c_ref[...], jnp.concatenate(fields, axis=0), 1, 1).astype(BF16)
            for part in range(2):
                row = 2 * (first + part) + group
                if row < BAND:
                    out_ref[:, row * CH : (row + 1) * CH] = made[:, part * CH : (part + 1) * CH]

    store.wait()
    most = pl.ds(0, MEMBERS - 1)
    for group in range(2):
        for source, target, sent in ((mine, everyone, sent_in), (share, score_ref, sent_out)):
            pltpu.make_async_copy(
                source.at[group, most], target.at[group, most], sent.at[group]
            ).wait()


def middle(live, area, s, c, x, truth, enct, dect, dec):
    quarter = (2, MEMBERS, FIELDS, NLON)
    return pl.pallas_call(
        middle_kernel,
        in_specs=[SMEM] * 2 + [VMEM] * 7,
        out_specs=[ANY, VMEM, VMEM],
        out_shape=[
            jax.ShapeDtypeStruct((1, FIELDS, BAND, NLON), BF16),
            jax.ShapeDtypeStruct(quarter, BF16),
            jax.ShapeDtypeStruct((BANDS * KM, WIDE), BF16),
        ],
        scratch_shapes=[
            pltpu.VMEM(quarter, BF16),
            pltpu.VMEM(quarter, BF16),
            pltpu.VMEM(quarter, BF16),
            pltpu.VMEM((2, MEMBERS, CH, NLON), BF16),
            pltpu.VMEM((len(TILES), FIELDS * 16, 128), F32),
            pltpu.VMEM((FIELDS, BAND, NLON), BF16),
            pltpu.SemaphoreType.DMA((1,)),
        ]
        + [pltpu.SemaphoreType.DMA((2,))] * 4,
        compiler_params=remote_params(3),
        name="middle",
    )(live, area, s, c, x, truth, enct, dect, dec)


def on_device(
    states, observed, band_rows, encoder_weight, mixing_weight, degree_gain, decoder_weight
):
    band = lax.axis_index("space")
    member = lax.axis_index("member")

    number = jnp.arange(BANDS, dtype=jnp.int32)
    point = jnp.arange(PTS, dtype=jnp.int32)
    point_band, point_row = point % BANDS, point // BANDS
    starts = jnp.sum(jnp.where(number[:, None] < point_band[None], band_rows[:, None], 0), axis=0)
    counts = jnp.sum(jnp.where(number[:, None] == point_band[None], band_rows[:, None], 0), axis=0)
    colatitude = jnp.minimum(starts + point_row, NLAT - 1).astype(F32) * (math.pi / (NLAT - 1))
    log_sine = jnp.log(jnp.maximum(jnp.sin(colatitude), 1e-30))
    live = (point_row < counts).astype(F32)
    zero = jnp.zeros_like(live)
    geo = jnp.stack([jnp.cos(colatitude), log_sine, live] + [zero] * 5)
    own_start = jnp.sum(jnp.where(number < band, band_rows, 0))
    own_count = jnp.sum(jnp.where(number == band, band_rows, 0))
    row = jnp.arange(16, dtype=jnp.int32)
    own_live = (row < own_count).astype(F32)
    own_lat = jnp.minimum(own_start + row, NLAT - 1).astype(F32) * (math.pi / (NLAT - 1))
    own_sine = jnp.sin(own_lat)
    own_weight = own_live * own_sine * (math.pi / (NLAT - 1) / NLON)
    own_area = 8.0 * own_sine * own_live

    c = fourier_table()
    diag = lax.dynamic_index_in_dim(jnp.asarray(diagonal_logs()), band, 0, keepdims=False)
    enc = encoder_weight
    enct = enc.T
    dec = decoder_weight
    dect = dec.T
    enc_wide = jnp.pad(enc, ((0, 128 - FIELDS), (0, 0)))
    enct_wide = enc_wide.T

    x = jnp.transpose(states[0], (1, 0, 2))
    synth, leg, legt = forward(
        own_weight, geo, diag, enc_wide, mixing_weight, degree_gain, c, x
    )
    synth = synth.reshape(BANDS * KM, WIDE)
    padded = jnp.pad(observed, ((0, 0), (0, 1), (0, 0)))
    truth = jnp.transpose(lax.dynamic_slice_in_dim(padded, member * 2, 2, 1), (1, 0, 2))
    prediction, score, grads = middle(own_live, own_area, synth, c, x, truth, enct, dect, dec)

    result = backward(
        own_weight, own_live, enct_wide, mixing_weight.T, degree_gain, enc, dec, c, score,
        leg, legt, grads.reshape(chunks(WIDE)),
    )
    return (prediction, result)


def solution(mesh):
    in_specs = (P("member", None, "space", None), P(None, "space", None), P(), P(), P(), P(), P())
    out_specs = (P("member", None, "space", None), P("member", None, "space", None))
    return jax.shard_map(
        on_device, mesh=mesh, in_specs=in_specs, out_specs=out_specs, check_vma=False
    )
```

```python
import math

import jax
import jax.numpy as jnp
import numpy as np
from jax import lax
from jax.experimental import pallas as pl
from jax.experimental.pallas import tpu as pltpu
from jax.sharding import PartitionSpec as P

NLAT = 361
LMAX = 360
NLON = 720
FIELDS = 73
CH = 128
BAND = 15
BANDS = 32
MEMBERS = 8
MDEV = 12
DEG = 384
PTS = 512
KM = 2 * MDEV
GROUPS = 3
GM = MDEV // GROUPS
GK = 2 * GM
MESH = pl.DeviceIdType.MESH
IDLE = (3, 9, 16, 22, 29)
BUSY = BANDS - len(IDLE)
FLAT = 1152
WIDE = BAND * CH

EPSILON = 1e-05
F32 = jnp.float32
BF16 = jnp.bfloat16


def dot(a, b, ca, cb):
    return lax.dot_general(a, b, (((ca,), (cb,)), ((), ())), preferred_element_type=F32)


SMEM = pl.BlockSpec(memory_space=pltpu.SMEM)
VMEM = pl.BlockSpec(memory_space=pltpu.VMEM)
ANY = pl.BlockSpec(memory_space=pl.ANY)
TILES = [(t * 128, min(128, NLON - t * 128)) for t in range(6)]


def group_orders():
    first = np.zeros((GROUPS, BANDS), np.int64)
    first[:2] = np.arange(2 * BANDS).reshape(2, BANDS) * GM
    rank = 2 * BANDS
    for owner in range(BANDS):
        idle = owner in IDLE
        first[2, owner] = (GROUPS * BANDS - 1 if idle else rank) * GM
        rank += 0 if idle else 1
    return first


def is_idle(device):
    found = device == IDLE[0]
    for other in IDLE[1:]:
        found = jnp.logical_or(found, device == other)
    return found


def first_of_group(group, device):
    skipped = sum(jnp.where(device > other, 1, 0) for other in IDLE)
    last = jnp.where(is_idle(device), GROUPS * BANDS - 1, 2 * BANDS + device - skipped)
    return jnp.where(group == 2, last, group * BANDS + device) * GM


def fourier_table():
    orders = group_orders()[:, :, None] + np.arange(GM)
    angle = 2.0 * np.pi * ((orders[..., None] * np.arange(NLON)) % NLON) / NLON
    live = (orders <= LMAX)[..., None]
    both = np.stack([np.where(live, np.cos(angle), 0.0), np.where(live, -np.sin(angle), 0.0)])
    both = both.transpose(1, 2, 0, 3, 4).reshape(BANDS * KM, NLON)
    return jnp.asarray(both.astype(np.float32), BF16)


def diagonal_logs():
    k = np.arange(1, BANDS * MDEV + 16, dtype=np.float64)
    steps = 0.5 * np.log((2.0 * k + 1.0) / (2.0 * k))
    logs = np.concatenate([[0.0], np.cumsum(steps)]).astype(np.float32) + np.float32(
        0.5 * math.log(0.5)
    )
    first = group_orders()
    orders = np.stack([first[0], first[1], first[2], first[2]])[:, :, None] + np.arange(GM)
    orders = orders.transpose(1, 0, 2).reshape(BANDS, 16)
    return np.broadcast_to(logs[orders][:, :, None], (BANDS, 16, 128))


def legendre_rows(geo_ref, diag_ref, table):
    band = lax.axis_index("space")
    cosine = jnp.broadcast_to(geo_ref[0:1, :], (16, PTS))
    log_sine = geo_ref[1:2, :]
    live = jnp.broadcast_to(geo_ref[2:3, :], (16, PTS))
    sublane = lax.broadcasted_iota(jnp.int32, (16, 128), 0)
    orders = jnp.where(
        sublane < GM,
        first_of_group(0, band) + sublane,
        jnp.where(
            sublane < 2 * GM,
            first_of_group(1, band) + sublane - GM,
            first_of_group(2, band) + jnp.bitwise_and(sublane, GM - 1),
        ),
    )
    order_f = orders.astype(F32)
    order_sq = order_f * order_f

    def wide(x):
        return jnp.concatenate([x] * (PTS // 128), axis=1)

    start = wide(diag_ref[...]) + wide(order_f) * log_sine

    def block(number, carry):
        first, second, log_scale = carry
        scale = jnp.exp(log_scale) * live
        for position in range(16):
            degree = number * 16 + position
            lf = jnp.full((16, 128), degree, jnp.int32).astype(F32)
            up = jnp.sqrt((4.0 * lf * lf - 1.0) / jnp.maximum(lf * lf - order_sq, 1.0))
            lb = lf - 1.0
            back = jnp.sqrt(
                jnp.maximum(lb * lb - order_sq, 0.0) / jnp.maximum(4.0 * lb * lb - 1.0, 1.0)
            )
            up = jnp.where(degree > orders, up, 0.0)
            onset = jnp.where(degree == orders, 1.0, 0.0)
            current = wide(up) * (cosine * first - wide(back) * second) + wide(onset)
            kept = jnp.where(jnp.full((16, PTS), degree, jnp.int32) <= LMAX, current * scale, 0.0)
            for part in range(PTS // 128):
                table[part, pl.ds(pl.multiple_of(degree * 16, 16), 16), :] = kept[
                    :, part * 128 : part * 128 + 128
                ]
            second = first
            first = current
        magnitude = jnp.maximum(jnp.abs(first), jnp.abs(second))
        factor = jnp.where(magnitude > 1.0, magnitude, 1.0)
        return first / factor, second / factor, log_scale + jnp.log(factor)

    zero = jnp.zeros((16, PTS), F32)
    lax.fori_loop(0, 23, block, (zero, zero, start))
    table[:, pl.ds(368 * 16, 16 * 16), :] = jnp.zeros((PTS // 128, 256, 128), F32)


def legendre_tables(table, leg, legt):
    def one(m, carry):
        for part in range(PTS // 128):
            lanes = slice(part * 128, part * 128 + 128)
            values = table[part, pl.ds(m, DEG, stride=16), :]
            leg[m, :, lanes] = values.astype(BF16)
            legt[m, lanes, :] = values.T.astype(BF16)
        return carry

    lax.fori_loop(0, MDEV, one, 0)


def window(row):
    start = row * FIELDS
    return start // 128 * 128, start % 128


def pack_windows(rows, value_of, put):
    low = spill = jnp.zeros((rows, 128), F32)
    at = 0
    for r in range(BAND):
        base, off = window(r)
        while at < base:
            put(at, low)
            low = spill
            at += 128
        value = value_of(r)
        moved = pltpu.roll(jnp.concatenate([value, jnp.zeros_like(value)], axis=1), off, 1)
        low = low + moved[:, :128]
        spill = moved[:, 128:]
    put(at, low)
    put(at + 128, spill)


def announce():
    band, member = lax.axis_index("space"), lax.axis_index("member")
    barrier = pltpu.get_barrier_semaphore()

    def signal(i, carry):
        peer = lax.rem(band + i, BANDS)
        pl.semaphore_signal(barrier, inc=1, device_id=(member, peer), device_id_type=MESH)
        return carry

    lax.fori_loop(1, BANDS, signal, 0)


def enter():
    pl.semaphore_wait(pltpu.get_barrier_semaphore(), BANDS - 1)


def send_in(source, target, group, sent, got):
    band, member = lax.axis_index("space"), lax.axis_index("member")

    def send(i, carry):
        peer = lax.rem(band + i, BANDS)

        def start():
            pltpu.make_async_remote_copy(
                src_ref=source.at[group, peer],
                dst_ref=target.at[group, band],
                send_sem=sent.at[group],
                recv_sem=got.at[group],
                device_id=(member, peer),
                device_id_type=MESH,
            ).start()

        if group == 2:
            pl.when(jnp.logical_not(is_idle(peer)))(start)
        else:
            start()
        return carry

    lax.fori_loop(1, BANDS, send, 0)

    def own():
        pltpu.make_async_copy(
            source.at[group, band], target.at[group, band], got.at[group]
        ).start()

    if group == 2:
        pl.when(jnp.logical_not(is_idle(band)))(own)
    else:
        own()


def send_out(source, target, group, sent, got):
    band, member = lax.axis_index("space"), lax.axis_index("member")

    def send(i, carry):
        peer = lax.rem(band + i, BANDS)
        pltpu.make_async_remote_copy(
            src_ref=source.at[group, peer],
            dst_ref=target.at[group, band],
            send_sem=sent.at[group],
            recv_sem=got.at[group],
            device_id=(member, peer),
            device_id_type=MESH,
        ).start()
        return carry

    lax.fori_loop(1, BANDS, send, 0)
    pltpu.make_async_copy(source.at[group, band], target.at[group, band], got.at[group]).start()


def wait_chunks(array, group, count, sem):
    part = array.at[group, pl.ds(0, count)]
    pltpu.make_async_copy(part, part, sem.at[group]).wait()


def wait_sent(first, second, sent_first, sent_second):
    for group in range(2):
        wait_chunks(first, group, BANDS - 1, sent_first)
        wait_chunks(second, group, BANDS - 1, sent_second)
    idle = is_idle(lax.axis_index("space"))

    @pl.when(idle)
    def _():
        wait_chunks(first, 2, BUSY, sent_first)

    @pl.when(jnp.logical_not(idle))
    def _():
        wait_chunks(first, 2, BUSY - 1, sent_first)
        wait_chunks(second, 2, BANDS - 1, sent_second)


def clear_idle(target):
    for owner in IDLE:
        target[2, owner] = jnp.zeros(target.shape[2:], BF16)


def each_busy_group(work):
    idle = is_idle(lax.axis_index("space"))

    def one_group(group, carry):
        pl.when(jnp.logical_not(jnp.logical_and(group == 2, idle)))(lambda: work(group))
        return carry

    lax.fori_loop(0, GROUPS, one_group, 0)


def gather_points(rows, points, order):
    for r in range(BAND):
        for k in range(2):
            got = rows[r, pl.ds(k * GM + order, BANDS, stride=GK), :]
            points[r * BANDS : (r + 1) * BANDS, k * 128 : (k + 1) * 128] = got.astype(BF16)


def scatter_points(synth, made, order):
    for r in range(BAND):
        for k in range(2):
            made[r, pl.ds(k * GM + order, BANDS, stride=GK), :] = synth[
                r * BANDS : (r + 1) * BANDS, k * 128 : (k + 1) * 128
            ]


def order_factor(order):
    return jnp.where(jnp.logical_or(order == 0, order == LMAX), 1.0, 2.0)


def forward_kernel(
    weight_ref, geo_ref, diag_ref, enc_ref, mix_ref, gain_ref, c_ref, x_ref,
    out_ref, leg_out, legt_out, z_ref, padded,
    table, leg, legt, arrived, rows, points, made, ready, sent_in, got_in, sent_out, got_out, kept
):
    band = lax.axis_index("space")
    announce()
    padded[...] = jnp.zeros(padded.shape, F32)
    for group in range(GROUPS):
        waves = c_ref[group * BANDS * GK : (group + 1) * BANDS * GK, :]

        def zonal(r):
            padded[:, :FIELDS] = dot(waves, x_ref[r], 1, 1) * weight_ref[r]
            return padded[...]

        def put_zonal(at, value):
            z_ref[group, :, :, at : at + 128] = value.reshape(BANDS, GK, 128).astype(BF16)

        pack_windows(BANDS * GK, zonal, put_zonal)
        if group == 0:
            enter()
        send_in(z_ref, arrived, group, sent_in, got_in)
    clear_idle(out_ref)
    legendre_rows(geo_ref, diag_ref, table)
    legendre_tables(table, leg, legt)
    save = pltpu.make_async_copy(leg, leg_out, kept.at[0])
    save_t = pltpu.make_async_copy(legt, legt_out, kept.at[1])
    save.start()
    save_t.start()
    points[...] = jnp.zeros((PTS, 256), BF16)

    def one_group(group):
        wait_chunks(arrived, group, BANDS, got_in)
        first_order = first_of_group(group, band)
        for r in range(BAND):
            base, off = window(r)
            pair = arrived[group, :, :, base : base + 256].astype(F32).reshape(BANDS * GK, 256)
            rows[r] = pltpu.roll(pair, (256 - off) % 256, 1)[:, :128]

        def one_order(order, carry):
            m = group * GM + order
            gather_points(rows, points, order)
            coeffs = dot(leg[m], points[...], 1, 0).astype(BF16)
            gain = padded_gain(gain_ref) * order_factor(first_order + order)
            filtered = []
            for k in range(2):
                fields = coeffs[:, k * 128 : k * 128 + FIELDS]
                channels = dot(fields, enc_ref[...], 1, 0).astype(BF16)
                filtered.append((dot(channels, mix_ref[...], 1, 0) * gain).astype(BF16))
            scatter_points(dot(legt[m], jnp.concatenate(filtered, axis=1), 1, 0), made, order)
            return carry

        lax.fori_loop(0, GM, one_order, 0)
        for r in range(BAND):
            ready[group, :, :, r * CH : (r + 1) * CH] = (
                made[r].reshape(BANDS, GK, CH).astype(BF16)
            )
        send_out(ready, out_ref, group, sent_out, got_out)

    each_busy_group(one_group)
    save.wait()
    save_t.wait()
    wait_sent(z_ref, ready, sent_in, sent_out)
    for group in range(GROUPS):
        wait_chunks(out_ref, group, BUSY if group == 2 else BANDS, got_out)


def padded_gain(gain_ref):
    rows = gain_ref.shape[0]
    return jnp.concatenate([gain_ref[...], jnp.zeros((DEG - rows, CH), F32)], axis=0)


def backward_kernel(
    weight_ref, live_ref, enct_ref, mix_ref, gain_ref, enc_ref, dec_ref, c_ref, g_ref,
    leg_in, legt_in, z_ref, out_ref,
    leg, legt, arrived, rows, points, made, ready, sent_in, got_in, sent_out, got_out, kept,
    returned, spread, local, wide_rows, final, stored,
):
    band = lax.axis_index("space")
    load = pltpu.make_async_copy(leg_in, leg, kept.at[0])
    load_t = pltpu.make_async_copy(legt_in, legt, kept.at[1])
    load.start()
    load_t.start()
    announce()
    enter()
    for group in range(GROUPS):
        send_in(z_ref, arrived, group, sent_in, got_in)
    clear_idle(returned)
    points[...] = jnp.zeros((PTS, 256), BF16)
    for r in range(BAND):
        score = g_ref[r % 2, r // 2]
        block = dot(dec_ref[...], score, 1, 0).astype(BF16)
        local[r] = score.astype(F32) + dot(enc_ref[...], block, 1, 0)
    load.wait()
    load_t.wait()

    def one_group(group):
        wait_chunks(arrived, group, BANDS, got_in)
        first_order = first_of_group(group, band)
        for r in range(BAND):
            rows[r] = (
                arrived[group, :, :, r * CH : (r + 1) * CH].astype(F32).reshape(BANDS * GK, CH)
            )

        def one_order(order, carry):
            m = group * GM + order
            gather_points(rows, points, order)
            grads = dot(leg[m], points[...], 1, 0)
            gain = padded_gain(gain_ref) * order_factor(first_order + order)
            back = []
            for k in range(2):
                scaled = (grads[:, k * 128 : (k + 1) * 128] * gain).astype(BF16)
                channels = dot(scaled, mix_ref[...], 1, 1).astype(BF16)
                back.append(dot(channels, enct_ref[...], 1, 0).astype(BF16))
            scatter_points(dot(legt[m], jnp.concatenate(back, axis=1), 1, 0), made, order)
            return carry

        lax.fori_loop(0, GM, one_order, 0)

        def put(at, value):
            ready[group, :, :, at : at + 128] = value.reshape(BANDS, GK, 128).astype(BF16)

        pack_windows(BANDS * GK, lambda r: made[r], put)
        send_out(ready, returned, group, sent_out, got_out)

    each_busy_group(one_group)
    for group in range(GROUPS):
        wait_chunks(returned, group, BUSY if group == 2 else BANDS, got_out)
        block = returned[group].astype(F32).reshape(BANDS * GK, FLAT).astype(BF16)
        part = dot(block, c_ref[group * BANDS * GK : (group + 1) * BANDS * GK, :], 0, 0)
        spread[...] = part if group == 0 else spread[...] + part
    for r in range(BAND):
        far = spread[r * FIELDS : (r + 1) * FIELDS, :] * weight_ref[r]
        result = (local[r] + far) * live_ref[r]
        for t, (start, size) in enumerate(TILES):
            wide_rows[t, pl.ds(r, FIELDS, stride=16), :size] = result[:, start : start + size]
    copies = []
    for part, (low, high) in enumerate(((0, 40), (40, FIELDS))):
        for t, (start, size) in enumerate(TILES):
            held = wide_rows[t, low * 16 : high * 16, :].reshape(high - low, 16, 128)
            final[low:high, :, start : start + size] = held[:, :BAND, :size].astype(BF16)
        copies.append(
            pltpu.make_async_copy(
                final.at[pl.ds(low, high - low)], out_ref.at[0, pl.ds(low, high - low)],
                stored.at[part],
            )
        )
        copies[-1].start()
    wait_sent(z_ref, ready, sent_in, sent_out)
    for copy in copies:
        copy.wait()


LEG = jax.ShapeDtypeStruct((MDEV, DEG, PTS), BF16)
LEGT = jax.ShapeDtypeStruct((MDEV, PTS, DEG), BF16)


def chunks(lanes):
    return (GROUPS, BANDS, GK, lanes)


def spectral_scratch(lanes_in, lanes_out):
    return [
        pltpu.VMEM(LEG.shape, BF16),
        pltpu.VMEM(LEGT.shape, BF16),
        pltpu.VMEM(chunks(lanes_in), BF16),
        pltpu.VMEM((BAND, BANDS * GK, 128), F32),
        pltpu.VMEM((PTS, 256), BF16),
        pltpu.VMEM((BAND, BANDS * GK, 128), F32),
        pltpu.VMEM(chunks(lanes_out), BF16),
    ] + [pltpu.SemaphoreType.DMA((GROUPS,))] * 4 + [pltpu.SemaphoreType.DMA((2,))]


def remote_params(collective):
    return pltpu.CompilerParams(
        collective_id=collective, vmem_limit_bytes=58 * 1024 * 1024, has_side_effects=True
    )


def forward(weight, geo, diag, enc, mix, gain, c, x):
    return pl.pallas_call(
        forward_kernel,
        in_specs=[SMEM] + [VMEM] * 7,
        out_specs=[VMEM, ANY, ANY],
        out_shape=[jax.ShapeDtypeStruct(chunks(WIDE), BF16), LEG, LEGT],
        scratch_shapes=[
            pltpu.VMEM(chunks(FLAT), BF16),
            pltpu.VMEM((BANDS * GK, 128), F32),
            pltpu.VMEM((PTS // 128, DEG * 16, 128), F32),
        ]
        + spectral_scratch(FLAT, WIDE),
        compiler_params=remote_params(1),
        name="forward",
    )(weight, geo, diag, enc, mix, gain, c, x)


def backward(weight, live, enct, mix, gain, enc, dec, c, score, leg, legt, z):
    return pl.pallas_call(
        backward_kernel,
        in_specs=[SMEM] * 2 + [VMEM] * 7 + [ANY] * 2 + [VMEM],
        out_specs=ANY,
        out_shape=jax.ShapeDtypeStruct((1, FIELDS, BAND, NLON), BF16),
        scratch_shapes=spectral_scratch(WIDE, FLAT)
        + [
            pltpu.VMEM(chunks(FLAT), BF16),
            pltpu.VMEM((FLAT, NLON), F32),
            pltpu.VMEM((BAND, FIELDS, NLON), F32),
            pltpu.VMEM((len(TILES), FIELDS * 16, 128), F32),
            pltpu.VMEM((FIELDS, BAND, NLON), BF16),
            pltpu.SemaphoreType.DMA((2,)),
        ],
        compiler_params=remote_params(2),
        name="backward",
    )(weight, live, enct, mix, gain, enc, dec, c, score, leg, legt, z)


def score_tile(p_ref, o_ref, out_ref, group, lanes, area):
    values = [p_ref[group, e, :, lanes].astype(F32) for e in range(MEMBERS)]
    truth = o_ref[group, :, lanes].astype(F32)

    def inverse(gap):
        return lax.rsqrt(jnp.sum(gap * gap, axis=0, keepdims=True) + EPSILON)

    weights = {}
    for e in range(MEMBERS):
        for f in range(e):
            weights[e, f] = weights[f, e] = inverse(values[e] - values[f]) * (area / MEMBERS)
    for e in range(MEMBERS):
        gap = values[e] - truth
        total = gap * (inverse(gap) * area)
        for f in range(MEMBERS):
            if f != e:
                total = total - (values[e] - values[f]) * weights[e, f]
        out_ref[group, e, :, lanes] = total.astype(BF16)


def middle_kernel(
    live_ref, area_ref, s_ref, c_ref, x_ref, o_ref, enct_ref, dect_ref, dec_ref,
    pred_ref, score_ref, out_ref,
    mine, everyone, share, slope, wide_rows, final, stored, sent_in, got_in, sent_out, got_out,
):
    band, member = lax.axis_index("space"), lax.axis_index("member")
    barrier = pltpu.get_barrier_semaphore()
    for i in range(1, MEMBERS):
        peer = lax.rem(member + i, MEMBERS)
        pl.semaphore_signal(barrier, inc=1, device_id=(peer, band), device_id_type=MESH)
    pl.semaphore_wait(barrier, MEMBERS - 1)

    def send(source, target, group, peer, sent, got):
        pltpu.make_async_remote_copy(
            src_ref=source.at[group, peer],
            dst_ref=target.at[group, member],
            send_sem=sent.at[group],
            recv_sem=got.at[group],
            device_id=(peer, band),
            device_id_type=MESH,
        ).start()

    def keep(source, target, group, got):
        pltpu.make_async_copy(
            source.at[group, member], target.at[group, member], got.at[group]
        ).start()

    def one_row(group, peer):
        row = 2 * peer + group
        held = jnp.minimum(row, BAND - 1)
        lanes = pl.ds(pl.multiple_of(held * CH, CH), CH)
        field = dot(s_ref[:, lanes], c_ref[...], 0, 0)
        live = live_ref[row]
        state = x_ref[held]
        hidden = (dot(enct_ref[...], state, 1, 0) * live).astype(BF16).astype(F32)
        cdf = 0.5 * (1.0 + lax.erf(field * (1.0 / math.sqrt(2.0))))
        gradient = cdf + field * jnp.exp(-0.5 * field * field) * (1.0 / math.sqrt(2.0 * math.pi))
        block = ((field * cdf + hidden) * live).astype(BF16)
        decoded = dot(dect_ref[...], block, 1, 0)
        result = (state.astype(F32) + decoded) * live
        mine[group, peer] = result.astype(BF16)
        slope[group, peer] = gradient.astype(BF16)
        for t, (start, size) in enumerate(TILES):
            wide_rows[t, pl.ds(row, FIELDS, stride=16), :size] = result[:, start : start + size]

    for group in range(2):

        def one_peer(i, carry):
            peer = lax.rem(member + i, MEMBERS)
            one_row(group, peer)
            send(mine, everyone, group, peer, sent_in, got_in)
            return carry

        lax.fori_loop(1, MEMBERS, one_peer, 0)
        one_row(group, member)
        keep(mine, everyone, group, got_in)

    for t, (start, size) in enumerate(TILES):
        held = wide_rows[t].reshape(FIELDS, 16, 128)
        final[:, :, start : start + size] = held[:, :BAND, :size].astype(BF16)
    store = pltpu.make_async_copy(final, pred_ref.at[0], stored.at[0])
    store.start()

    def score_group(group, carry):
        pltpu.make_async_copy(mine.at[group], everyone.at[group], got_in.at[group]).wait()
        area = area_ref[2 * member + group]

        def one_tile(t, inner):
            lanes = pl.ds(pl.multiple_of(t * 128, 128), 128)
            score_tile(everyone, o_ref, share, group, lanes, area)
            return inner

        lax.fori_loop(0, 5, one_tile, 0)
        score_tile(everyone, o_ref, share, group, pl.ds(640, NLON - 640), area)

        def one_peer(i, inner):
            send(share, score_ref, group, lax.rem(member + i, MEMBERS), sent_out, got_out)
            return inner

        lax.fori_loop(1, MEMBERS, one_peer, 0)
        keep(share, score_ref, group, got_out)
        return carry

    lax.fori_loop(0, 2, score_group, 0)

    for group in range(2):
        pltpu.make_async_copy(share.at[group], score_ref.at[group], got_out.at[group]).wait()
        for first in range(0, MEMBERS, 2):
            fields = []
            for peer in (first, first + 1):
                block = dot(dec_ref[...], score_ref[group, peer], 1, 0)
                fields.append((block * slope[group, peer].astype(F32)).astype(BF16))
            made = dot(c_ref[...], jnp.concatenate(fields, axis=0), 1, 1).astype(BF16)
            for part in range(2):
                row = 2 * (first + part) + group
                if row < BAND:
                    out_ref[:, row * CH : (row + 1) * CH] = made[:, part * CH : (part + 1) * CH]

    store.wait()
    most = pl.ds(0, MEMBERS - 1)
    for group in range(2):
        for source, target, sent in ((mine, everyone, sent_in), (share, score_ref, sent_out)):
            pltpu.make_async_copy(
                source.at[group, most], target.at[group, most], sent.at[group]
            ).wait()


def middle(live, area, s, c, x, truth, enct, dect, dec):
    quarter = (2, MEMBERS, FIELDS, NLON)
    return pl.pallas_call(
        middle_kernel,
        in_specs=[SMEM] * 2 + [VMEM] * 7,
        out_specs=[ANY, VMEM, VMEM],
        out_shape=[
            jax.ShapeDtypeStruct((1, FIELDS, BAND, NLON), BF16),
            jax.ShapeDtypeStruct(quarter, BF16),
            jax.ShapeDtypeStruct((BANDS * KM, WIDE), BF16),
        ],
        scratch_shapes=[
            pltpu.VMEM(quarter, BF16),
            pltpu.VMEM(quarter, BF16),
            pltpu.VMEM(quarter, BF16),
            pltpu.VMEM((2, MEMBERS, CH, NLON), BF16),
            pltpu.VMEM((len(TILES), FIELDS * 16, 128), F32),
            pltpu.VMEM((FIELDS, BAND, NLON), BF16),
            pltpu.SemaphoreType.DMA((1,)),
        ]
        + [pltpu.SemaphoreType.DMA((2,))] * 4,
        compiler_params=remote_params(3),
        name="middle",
    )(live, area, s, c, x, truth, enct, dect, dec)


def on_device(
    states, observed, band_rows, encoder_weight, mixing_weight, degree_gain, decoder_weight
):
    band = lax.axis_index("space")
    member = lax.axis_index("member")

    number = jnp.arange(BANDS, dtype=jnp.int32)
    point = jnp.arange(PTS, dtype=jnp.int32)
    point_band, point_row = point % BANDS, point // BANDS
    starts = jnp.sum(jnp.where(number[:, None] < point_band[None], band_rows[:, None], 0), axis=0)
    counts = jnp.sum(jnp.where(number[:, None] == point_band[None], band_rows[:, None], 0), axis=0)
    colatitude = jnp.minimum(starts + point_row, NLAT - 1).astype(F32) * (math.pi / (NLAT - 1))
    log_sine = jnp.log(jnp.maximum(jnp.sin(colatitude), 1e-30))
    live = (point_row < counts).astype(F32)
    zero = jnp.zeros_like(live)
    geo = jnp.stack([jnp.cos(colatitude), log_sine, live] + [zero] * 5)
    own_start = jnp.sum(jnp.where(number < band, band_rows, 0))
    own_count = jnp.sum(jnp.where(number == band, band_rows, 0))
    row = jnp.arange(16, dtype=jnp.int32)
    own_live = (row < own_count).astype(F32)
    own_lat = jnp.minimum(own_start + row, NLAT - 1).astype(F32) * (math.pi / (NLAT - 1))
    own_sine = jnp.sin(own_lat)
    own_weight = own_live * own_sine * (math.pi / (NLAT - 1) / NLON)
    own_area = 8.0 * own_sine * own_live

    c = fourier_table()
    diag = lax.dynamic_index_in_dim(jnp.asarray(diagonal_logs()), band, 0, keepdims=False)
    enc = encoder_weight
    enct = enc.T
    dec = decoder_weight
    dect = dec.T
    enc_wide = jnp.pad(enc, ((0, 128 - FIELDS), (0, 0)))
    enct_wide = enc_wide.T

    x = jnp.transpose(states[0], (1, 0, 2))
    synth, leg, legt = forward(
        own_weight, geo, diag, enc, mixing_weight, degree_gain, c, x
    )
    synth = synth.reshape(BANDS * KM, WIDE)
    padded = jnp.pad(observed, ((0, 0), (0, 1), (0, 0)))
    truth = jnp.transpose(lax.dynamic_slice_in_dim(padded, member * 2, 2, 1), (1, 0, 2))
    prediction, score, grads = middle(own_live, own_area, synth, c, x, truth, enct, dect, dec)

    result = backward(
        own_weight, own_live, enct_wide, mixing_weight, degree_gain, enc, dec, c, score,
        leg, legt, grads.reshape(chunks(WIDE)),
    )
    return (prediction, result)


def solution(mesh):
    in_specs = (P("member", None, "space", None), P(None, "space", None), P(), P(), P(), P(), P())
    out_specs = (P("member", None, "space", None), P("member", None, "space", None))
    return jax.shard_map(
        on_device, mesh=mesh, in_specs=in_specs, out_specs=out_specs, check_vma=False
    )
```
